512 devices in a mesh: los: 32 (over z, x), sky: 16 (over y, core).
Axes of the slice: x: 4, y: 8, z: 8, core: 2. Of those that a mesh axis runs over, the one named last changes fastest.
Arguments:
- part_cell: int32 [3, 2097152], P(None, ('los', 'sky')), may hold values from 0 to 127, as said below
- part_frac: float32 [3, 2097152], P(None, ('los', 'sky')), may hold values from 0 to 1
- los_offset: int32 [2097152], P(('los', 'sky')), may hold values from -32 to 32
- block_dest: int32 [16384], P(('los', 'sky')), may hold values from 0 to 31, as said below
- block_count: int32 [16384], P(('los', 'sky')), may hold values from 96 to 128, as said below
- selection: float32 [128, 64, 128], P('los', 'sky'), may hold values from 0.3 to 3
- galaxy_counts: int32 [128, 64, 128], P('los', 'sky'), may hold values from 0 to 5
- bias_exp: float32 [128], P('los'), may hold values from 1.2 to 2.2
- rsd_factor: float32 [128], P('los'), may hold values from 0.5 to 2
Outputs:
- grad_pos: float32 [3, 2097152], P(None, ('los', 'sky'))
- grad_vel: float32 [2097152], P(('los', 'sky'))
The draws below stay inside these ranges and needn't reach their ends.
Inputs may be any that keep to these rules, and one draw needn't show every extreme that they name: Component 1 of a particle lies in the first-sky cells of its own device's columns, and (part_cell[0] + los_offset) mod 128 lies in cells block_dest * 4 to block_dest * 4 + 3 of the particle's block, for every slot. `block_dest`: the 32 blocks of one device name any slab at most 2 times, and on every device some slab is named exactly 2 times. `block_count`: A block's live particles are its first slots; every device has a full block.
All inputs are finite; a program needn't handle non-finite values.
Results may differ from the reference program's by a relative error of at most 0.000098.
Values sent between devices are 32-bit elements; how exact they have to be, the bound alone decides.
A program may use at most 64 MiB of HBM per device.

```python
import math
import jax
import jax.numpy as jnp
from jax import lax

CL = 4
CA = 4
NB = 128
NBK = 32
BLK = 128
MAXOFF = 32
PART = 2097152
NL = 128
NA = 64
N_LOS = 32
N_SKY = 16


def routing(key):
    subkeys = jax.random.split(jax.random.fold_in(key, 11), 10)
    devices = N_LOS * N_SKY
    capacity = 2 * NBK // N_LOS
    slot_count = N_LOS * capacity
    slot_dest = jnp.arange(slot_count, dtype=jnp.int32) // capacity
    favour = jax.random.randint(subkeys[0], (N_LOS,), 0, 2048)
    hottest = jax.random.randint(subkeys[1], (devices,), 0, N_LOS)
    jitter = jax.random.randint(subkeys[2], (devices, slot_count), 0, 1024)
    scores = favour[slot_dest][None, :] + jitter + jnp.where(slot_dest[None, :] == hottest[:, None], 4096, 0)
    scores = scores * slot_count + jnp.arange(slot_count, dtype=jnp.int32)[None, :]
    top_scores, chosen = lax.top_k(scores, NBK)
    shuffle = jax.random.randint(subkeys[3], (devices, NBK), 0, 1 << 20) * NBK + jnp.arange(NBK, dtype=jnp.int32)[None, :]
    reorder = jnp.argsort(shuffle, axis=1)
    chosen = jnp.take_along_axis(chosen, reorder, axis=1)
    target_slab = (chosen // capacity).astype(jnp.int32)
    counts = jax.random.randint(subkeys[4], (devices, NBK), max(1, 3 * BLK // 4), BLK + 1)
    full_at = jax.random.randint(subkeys[5], (devices,), 0, NBK)
    counts = jnp.where(jnp.arange(NBK, dtype=jnp.int32)[None, :] == full_at[:, None], BLK, counts)
    grid_shape = (devices, NBK, BLK)
    red_cell = target_slab[:, :, None] * CL + jax.random.randint(subkeys[6], grid_shape, 0, CL)
    offset = jax.random.randint(subkeys[7], grid_shape, -MAXOFF, MAXOFF + 1)
    los_cell = jnp.mod(red_cell - offset, CL * N_LOS)
    sky_index = jnp.arange(devices, dtype=jnp.int32) % N_SKY
    sky_cell = sky_index[:, None, None] * CA + jax.random.randint(subkeys[8], grid_shape, 0, CA)
    deep_cell = jax.random.randint(subkeys[9], grid_shape, 0, NB)
    cells = jnp.stack([los_cell, sky_cell, deep_cell]).reshape(3, -1).astype(jnp.int32)
    return (cells, offset.reshape(-1).astype(jnp.int32), target_slab.reshape(-1), counts.reshape(-1).astype(jnp.int32))


def draw_part_cell(key, part):
    return routing(key)[0]


def draw_los_offset(key, part):
    return routing(key)[1]


def draw_block_dest(key, part):
    return routing(key)[2]


def draw_block_count(key, part):
    return routing(key)[3]


def set_ends(array, key, low, largest):
    longest = array.shape.index(max(array.shape))
    spots = []
    for shift in (0, 1):
        where = [jax.random.randint(jax.random.fold_in(key, axis), (), 0, length) for axis, length in enumerate(array.shape)]
        where[longest] = (where[longest] + shift) % array.shape[longest]
        spots.append(tuple(where))
    return array.at[spots[0]].set(low).at[spots[1]].set(largest)


def block_levels(rng, shape, shards, least, high):
    def one(axis_at, parts):
        steps = jax.random.uniform(jax.random.fold_in(jax.random.fold_in(rng, 6), axis_at), (parts,), jnp.float32, least / len(shards), high / len(shards))
        return jnp.repeat(jnp.exp(steps), shape[axis_at] // parts).reshape((-1,) + (1,) * (len(shape) - axis_at - 1))

    level = one(*shards[0])
    for cut in shards[1:]:
        level = level * one(*cut)
    return level


def setup_inputs(seed: int = 0) -> dict:
    arg_keys = jax.random.split(jax.random.key(seed), 10)
    part_cell = draw_part_cell(jax.random.fold_in(arg_keys[9], 71), 0)
    part_frac = jnp.clip(1.0 * jax.random.uniform(arg_keys[1], (3, PART), jnp.float32) ** block_levels(arg_keys[1], (3, PART), ((1, 512),), -0.2, 0.2), 0.0, 1.0)
    los_offset = draw_los_offset(jax.random.fold_in(arg_keys[9], 71), 0)
    block_dest = draw_block_dest(jax.random.fold_in(arg_keys[9], 71), 0)
    block_count = draw_block_count(jax.random.fold_in(arg_keys[9], 71), 0)
    selection = jnp.clip(jnp.exp(math.log(3.0) - 2.3025851 * jax.random.uniform(arg_keys[5], (NL, NA, NB), jnp.float32) ** block_levels(arg_keys[5], (NL, NA, NB), ((0, 32), (1, 16)), -0.2, 0.2)), 0.3, 3.0)
    galaxy_counts = set_ends(jax.random.randint(arg_keys[6], (NL, NA, NB), 0, 6), jax.random.fold_in(arg_keys[6], 1), 0, 5).astype(jnp.int32)
    bias_exp = jnp.clip(jnp.exp(math.log(2.2) - 0.6061358 * jax.random.uniform(arg_keys[7], (NL,), jnp.float32) ** block_levels(arg_keys[7], (NL,), ((0, 32),), -0.2, 0.2)), 1.2, 2.2)
    rsd_factor = jnp.clip(jnp.exp(math.log(2.0) - 1.3862944 * jax.random.uniform(arg_keys[8], (NL,), jnp.float32) ** block_levels(arg_keys[8], (NL,), ((0, 32),), -0.2, 0.2)), 0.5, 2.0)
    return dict(part_cell=part_cell, part_frac=part_frac, los_offset=los_offset, block_dest=block_dest, block_count=block_count, selection=selection, galaxy_counts=galaxy_counts, bias_exp=bias_exp, rsd_factor=rsd_factor)


def corner_bits():
    return [(los_bit, sky_bit, deep_bit) for los_bit in (0, 1) for sky_bit in (0, 1) for deep_bit in (0, 1)]


def factor(fraction, bit):
    return fraction if bit else 1.0 - fraction


def slope(bit):
    return 1.0 if bit else -1.0


def reference(part_cell, part_frac, los_offset, block_dest, block_count, selection, galaxy_counts, bias_exp, rsd_factor):
    slot_index = jnp.arange(BLK, dtype=jnp.int32)
    alive = (slot_index[None, :] < block_count[:, None]).astype(jnp.float32).reshape(-1)
    dest_each = jnp.repeat(block_dest, BLK).astype(jnp.int32)
    red_cell = (dest_each * CL + jnp.mod(part_cell[0] + los_offset, CL)).astype(jnp.int32)
    sky_cell = part_cell[1]
    deep_cell = part_cell[2]
    frac_los = part_frac[0]
    frac_sky = part_frac[1]
    frac_deep = part_frac[2]
    density = jnp.zeros((NL * NA * NB,), jnp.float32)
    flat_list = []
    slope_list = []
    for bits in corner_bits():
        flat_index = ((jnp.mod(red_cell + bits[0], NL) * NA + jnp.mod(sky_cell + bits[1], NA)) * NB + jnp.mod(deep_cell + bits[2], NB)).astype(jnp.int32)
        weight_los = factor(frac_los, bits[0])
        weight_sky = factor(frac_sky, bits[1])
        weight_deep = factor(frac_deep, bits[2])
        weight = weight_los * weight_sky * weight_deep
        density = density.at[flat_index].add(weight * alive)
        flat_list.append(flat_index)
        slope_list.append((slope(bits[0]) * weight_sky * weight_deep, weight_los * slope(bits[1]) * weight_deep, weight_los * weight_sky * slope(bits[2])))
    density = density.reshape(NL, NA, NB)
    shifted = density + 0.5
    exponent = bias_exp[:, None, None]
    intensity = selection * jnp.exp(exponent * jnp.log(shifted))
    cotangent = (1.0 - galaxy_counts.astype(jnp.float32) / intensity) * exponent * intensity / shifted
    flat_field = cotangent.reshape(-1)
    grad_los = jnp.zeros((PART,), jnp.float32)
    grad_sky = jnp.zeros((PART,), jnp.float32)
    grad_deep = jnp.zeros((PART,), jnp.float32)
    for flat_index, slopes in zip(flat_list, slope_list):
        picked = flat_field[flat_index]
        grad_los = grad_los + slopes[0] * picked
        grad_sky = grad_sky + slopes[1] * picked
        grad_deep = grad_deep + slopes[2] * picked
    grad_pos = jnp.stack([grad_los, grad_sky, grad_deep]) * alive[None, :]
    grad_vel = rsd_factor[red_cell] * grad_los * alive
    return grad_pos, grad_vel
```

```python
import functools

import jax
import jax.numpy as jnp
from jax import lax
from jax.experimental import pallas as pl
from jax.experimental.pallas import tpu as pltpu
from jax.sharding import PartitionSpec as P

MESH = pl.DeviceIdType.MESH
F32 = jnp.float32
BF16 = jnp.bfloat16
LANES = 128
X = 4


def row_iota():
    return lax.broadcasted_iota(jnp.int32, (8, LANES), 0)


def split(values):
    high = values.astype(BF16)
    low = (values - high.astype(F32)).astype(BF16)
    return jnp.concatenate([high, low], axis=0)


def to_slots(dest, counts, cell, frac, off, slots, place, seen):
    sky_base = lax.axis_index("sky") * 4
    row = row_iota()
    empty = jnp.where(row == 0, -8.0, 0.0)
    for i in range(slots.shape[0]):
        slots[i] = empty
    for i in range(seen.shape[0]):
        seen[i] = 0
    lane = lax.broadcasted_iota(jnp.int32, (1, LANES), 1)
    for b in range(dest.shape[0]):
        lanes = slice(b * LANES, (b + 1) * LANES)
        los = jnp.where(lane < counts[b], (cell[0:1, lanes] + off[b : b + 1, :]) & 3, -8)
        slab = dest[b]
        rank = seen[slab]
        seen[slab] = rank + 1
        slot = slab * 2 + rank
        place[b] = slot
        cells = jnp.concatenate([los, cell[1:2, lanes] - sky_base, cell[2:3, lanes]], axis=0)
        slots[slot, 0:3] = cells.astype(F32)
        slots[slot, 3:6] = frac[:, lanes]


def from_slots(place, pulled, out_pos, out_vel):
    for b in range(place.shape[0]):
        values = pulled[place[b]]
        out_pos[:, b * LANES : (b + 1) * LANES] = values[:3]
        out_vel[b : b + 1, :] = values[3:]


def slot_rows(slots, i):
    return [slots[i, r : r + 1] for r in range(6)]


def one_hot_deep(deep):
    iota = lax.broadcasted_iota(jnp.int32, (LANES, LANES), 0).astype(F32)
    return jnp.where(iota == deep, 1.0, 0.0).astype(BF16)


def kernel(
    bias,
    rsd,
    slots,
    selection,
    galaxies,
    pulled,
    hot,
    grid,
    grid_side,
    rx,
    rx_side,
    total,
    rz,
    field,
    field_side,
    rates,
    send_x,
    recv_x,
    send_side,
    recv_side,
    send_z,
    recv_z,
    send_cz,
    recv_cz,
    send_f,
    recv_f,
    send_fs,
    recv_fs,
    send_rz,
    recv_rz,
    send_rx,
    recv_rx,
):
    z_size = grid.shape[1]
    sky_size = lax.axis_size("sky")
    los_here = lax.axis_index("los")
    sky_here = lax.axis_index("sky")
    z_here = los_here // X
    x_here = los_here % X
    sky_up = (sky_here + 1) % sky_size
    sky_down = (sky_here + sky_size - 1) % sky_size

    def x_peer(k):
        return z_here * X + (x_here + k) % X

    def z_peer(k):
        return ((z_here + k) % z_size) * X + x_here

    barrier = pltpu.get_barrier_semaphore()
    for k in range(X):
        if k:
            pl.semaphore_signal(
                barrier, inc=1, device_id=(x_peer(k), sky_here), device_id_type=MESH
            )
        for sky_to in (sky_up, sky_down):
            pl.semaphore_signal(barrier, inc=1, device_id=(x_peer(k), sky_to), device_id_type=MESH)
    for k in range(1, z_size):
        pl.semaphore_signal(barrier, inc=1, device_id=(z_peer(k), sky_here), device_id_type=MESH)

    row4 = lax.broadcasted_iota(jnp.int32, (4, LANES), 0)

    def by_row(scalars):
        value = jnp.full((4, LANES), scalars[3], F32)
        for i in (0, 1, 2):
            value = jnp.where(row4 == i, scalars[i], value)
        return value

    rates[x_here, z_here] = by_row(rsd)
    row = row_iota().astype(F32)

    def paint(t, previous):
        tables, hots = [], []
        for slot in (0, 1):
            los, sky, deep, f_los, f_sky, f_deep = slot_rows(slots, t * 2 + slot)
            h_los = jnp.where(row == los, 1.0 - f_los, 0.0) + jnp.where(row == los + 1, f_los, 0.0)
            h_sky = jnp.where(row == sky, 1.0 - f_sky, 0.0) + jnp.where(row == sky + 1, f_sky, 0.0)
            lower, upper = h_los * (1.0 - f_deep), h_los * f_deep
            parts = []
            for s in range(5):
                parts += [h_sky[s : s + 1] * lower, h_sky[s : s + 1] * upper]
            tables.append(split(jnp.concatenate(parts, axis=0)))
            one_hot = one_hot_deep(deep)
            hot[t, :, slot * LANES : (slot + 1) * LANES] = one_hot
            hots.append(one_hot)
        result = lax.dot_general(
            jnp.concatenate(tables, axis=1),
            jnp.concatenate(hots, axis=1),
            (((1,), (1,)), ((), ())),
            preferred_element_type=F32,
        )
        result = result[:80] + result[80:]
        planes = []
        for s in range(5):
            lower, upper = result[s * 16 : s * 16 + 8], result[s * 16 + 8 : s * 16 + 16]
            planes.append(lower + pltpu.roll(upper, 1, 1))
        return planes

    def paint_step(step, previous):
        for i in range(2):
            z = step * 2 + i
            for x in range(X):
                planes = paint(z * X + x, previous)
                for s in range(5):
                    carried = jnp.where(row == 0, pltpu.roll(previous[s], 4, 0), 0.0)
                    whole = (planes[s] + carried)[:4]
                    if s < 4:
                        grid[x, z, s] = whole
                    else:
                        grid_side[x, z] = whole
                previous = planes
        return tuple(previous)

    zero = jnp.zeros((8, LANES), F32)
    last = lax.fori_loop(0, z_size // 2, paint_step, (zero,) * 5)
    for s in range(5):
        carried = jnp.where(row == 0, pltpu.roll(last[s], 4, 0), 0.0)[:4]
        if s < 4:
            grid[0, 0, s] = grid[0, 0, s] + carried
        else:
            grid_side[0, 0] = grid_side[0, 0] + carried

    pl.semaphore_wait(barrier, 3 + 2 * X + z_size - 1)

    def remote(src, dst, send_sem, recv_sem, los_to, sky_to):
        return pltpu.make_async_remote_copy(
            src_ref=src,
            dst_ref=dst,
            send_sem=send_sem,
            recv_sem=recv_sem,
            device_id=(los_to, sky_to),
            device_id_type=MESH,
        )

    x_copies, side_copies = {}, {}
    for k in (2, 1, 3, 0):
        x_to = (x_here + k) % X
        if k:
            x_copies[k] = remote(
                grid.at[x_to], rx.at[k - 1], send_x.at[k - 1], recv_x.at[k - 1], x_peer(k), sky_here
            )
            x_copies[k].start()
        side_copies[k] = remote(
            grid_side.at[x_to],
            rx_side.at[k],
            send_side.at[k],
            recv_side.at[k],
            x_peer(k),
            sky_up,
        )
        side_copies[k].start()
    rate_z = {}
    for k in range(1, z_size):
        rate_z[k] = remote(
            rates.at[x_here, z_here],
            rates.at[x_here, z_here],
            send_rz.at[k - 1],
            recv_rz.at[k - 1],
            z_peer(k),
            sky_here,
        )
        rate_z[k].start()
    for k in range(X):
        if k:
            x_copies[k].wait_recv()
        side_copies[k].wait_recv()

    def gather_x(z):
        for s in range(4):
            value = grid[x_here, z, s]
            for k in range(1, X):
                value = value + rx[k - 1, z, s]
            if s == 0:
                for k in range(X):
                    value = value + rx_side[k, z]
            total[z, s] = value

    order = sorted(range(1, z_size), key=lambda k: -min(k, z_size - k))
    z_copies = {}
    for k in order:
        z_to = (z_here + k) % z_size
        gather_x(z_to)
        z_copies[k] = remote(
            total.at[z_to], rz.at[k - 1], send_z.at[k - 1], recv_z.at[k - 1], z_peer(k), sky_here
        )
        z_copies[k].start()
    gather_x(z_here)

    for k in range(1, z_size):
        rate_z[k].wait_recv()
    rate_x = {}
    for k in range(1, X):
        rate_x[k] = remote(
            rates.at[x_here],
            rates.at[x_here],
            send_rx.at[k - 1],
            recv_rx.at[k - 1],
            x_peer(k),
            sky_here,
        )
        rate_x[k].start()

    exponent = by_row(bias)
    for k in range(1, z_size):
        z_copies[k].wait_recv()
    for s in range(4):
        density = total[z_here, s]
        for k in range(1, z_size):
            density = density + rz[k - 1, s]
        mean = jnp.concatenate([selection[l, s : s + 1] for l in range(4)], axis=0)
        seen = jnp.concatenate([galaxies[l, s : s + 1] for l in range(4)], axis=0).astype(F32)
        shifted = density + 0.5
        intensity = mean * jnp.exp(exponent * jnp.log(shifted))
        field[x_here, z_here, s] = (1.0 - seen / intensity) * exponent * intensity / shifted

    cz_copies = {}
    for k in order:
        cz_copies[k] = remote(
            field.at[x_here, z_here],
            field.at[x_here, z_here],
            send_cz.at[k - 1],
            recv_cz.at[k - 1],
            z_peer(k),
            sky_here,
        )
        cz_copies[k].start()
    f_copies, fs_copies = {}, {}
    for j in sorted(range(z_size), key=lambda k: min(k, z_size - k)):
        if j:
            cz_copies[j].wait_recv()
        z_from = (z_here + z_size - j) % z_size
        for k in (2, 1, 3, 0):
            if k:
                f_copies[j, k] = remote(
                    field.at[x_here, z_from],
                    field.at[x_here, z_from],
                    send_f.at[j, k - 1],
                    recv_f.at[j, k - 1],
                    x_peer(k),
                    sky_here,
                )
                f_copies[j, k].start()
            fs_copies[j, k] = remote(
                field.at[x_here, z_from, 0],
                field_side.at[x_here, z_from],
                send_fs.at[j, k],
                recv_fs.at[j, k],
                x_peer(k),
                sky_down,
            )
            fs_copies[j, k].start()
    for k in range(1, X):
        rate_x[k].wait_recv()
    for j, k in f_copies:
        f_copies[j, k].wait_recv()
    for j, k in fs_copies:
        fs_copies[j, k].wait_recv()

    def pull(z, x):
        t = z * X + x
        z_next, x_next = (z, x + 1) if x + 1 < X else (lax.rem(z + 1, z_size), 0)
        rows = []
        for s in range(5):
            if s < 4:
                value = jnp.concatenate([field[x, z, s], field[x_next, z_next, s]], axis=0)
            else:
                value = jnp.concatenate([field_side[x, z], field_side[x_next, z_next]], axis=0)
            rows += [value, pltpu.roll(value, LANES - 1, 1)]
        picked = jnp.dot(
            split(jnp.concatenate(rows, axis=0)), hot[t], preferred_element_type=F32
        )
        picked = picked[:80] + picked[80:]
        rate = jnp.concatenate([rates[x, z], jnp.zeros((4, LANES), F32)], axis=0)
        for slot in (0, 1):
            los, sky, deep, f_los, f_sky, f_deep = slot_rows(slots, t * 2 + slot)
            at, above = row == los, row == los + 1
            h_los = jnp.where(at, 1.0 - f_los, 0.0) + jnp.where(above, f_los, 0.0)
            d_los = jnp.where(above, 1.0, 0.0) - jnp.where(at, 1.0, 0.0)
            r_los = jnp.where(at, rate, 0.0)
            at, above = row == sky, row == sky + 1
            h_sky = jnp.where(at, 1.0 - f_sky, 0.0) + jnp.where(above, f_sky, 0.0)
            d_sky = jnp.where(above, 1.0, 0.0) - jnp.where(at, 1.0, 0.0)
            lanes = slice(slot * LANES, (slot + 1) * LANES)
            val, val_sky, val_deep = zero, zero, zero
            for s in range(5):
                here = picked[s * 16 : s * 16 + 8, lanes]
                step = picked[s * 16 + 8 : s * 16 + 16, lanes] - here
                mixed = here + f_deep * step
                val = val + h_sky[s : s + 1] * mixed
                val_sky = val_sky + d_sky[s : s + 1] * mixed
                val_deep = val_deep + h_sky[s : s + 1] * step
            g_los = jnp.sum(d_los * val, axis=0, keepdims=True)
            g_sky = jnp.sum(h_los * val_sky, axis=0, keepdims=True)
            g_deep = jnp.sum(h_los * val_deep, axis=0, keepdims=True)
            speed = jnp.sum(r_los, axis=0, keepdims=True) * g_los
            pulled[t * 2 + slot] = jnp.concatenate([g_los, g_sky, g_deep, speed], axis=0)

    def pull_step(step, unused):
        for i in range(2):
            for x in range(X):
                pull(step * 2 + i, x)
        return unused

    lax.fori_loop(0, z_size // 2, pull_step, 0)

    for copies in (
        x_copies,
        side_copies,
        rate_z,
        z_copies,
        rate_x,
        cz_copies,
        f_copies,
        fs_copies,
    ):
        for copy in copies.values():
            copy.wait_send()


def on_device(
    part_cell,
    part_frac,
    los_offset,
    block_dest,
    block_count,
    selection,
    galaxy_counts,
    bias_exp,
    rsd_factor,
):
    los_size = lax.axis_size("los")
    z_size = los_size // X
    blocks = block_dest.shape[0]
    vmem = pl.BlockSpec(memory_space=pltpu.VMEM)
    smem = pl.BlockSpec(memory_space=pltpu.SMEM)
    dma = pltpu.SemaphoreType.DMA
    slots, place = pl.pallas_call(
        to_slots,
        out_shape=(
            jax.ShapeDtypeStruct((2 * los_size, 8, LANES), F32),
            jax.ShapeDtypeStruct((blocks,), jnp.int32),
        ),
        in_specs=[smem] * 2 + [vmem] * 3,
        out_specs=(vmem, smem),
        scratch_shapes=[pltpu.SMEM((los_size,), jnp.int32)],
        name="to_slots",
    )(block_dest, block_count, part_cell, part_frac, los_offset.reshape(blocks, LANES))
    pulled = pl.pallas_call(
        kernel,
        out_shape=jax.ShapeDtypeStruct((2 * los_size, 4, LANES), F32),
        in_specs=[smem] * 2 + [vmem] * 3,
        out_specs=vmem,
        scratch_shapes=[
            pltpu.VMEM((los_size, LANES, 2 * LANES), BF16),
            pltpu.VMEM((X, z_size, 4, 4, LANES), F32),
            pltpu.VMEM((X, z_size, 4, LANES), F32),
            pltpu.VMEM((X - 1, z_size, 4, 4, LANES), F32),
            pltpu.VMEM((X, z_size, 4, LANES), F32),
            pltpu.VMEM((z_size, 4, 4, LANES), F32),
            pltpu.VMEM((z_size - 1, 4, 4, LANES), F32),
            pltpu.VMEM((X, z_size, 4, 4, LANES), F32),
            pltpu.VMEM((X, z_size, 4, LANES), F32),
            pltpu.VMEM((X, z_size, 4, LANES), F32),
            dma((X - 1,)),
            dma((X - 1,)),
            dma((X,)),
            dma((X,)),
            dma((z_size - 1,)),
            dma((z_size - 1,)),
            dma((z_size - 1,)),
            dma((z_size - 1,)),
            dma((z_size, X - 1)),
            dma((z_size, X - 1)),
            dma((z_size, X)),
            dma((z_size, X)),
            dma((z_size - 1,)),
            dma((z_size - 1,)),
            dma((X - 1,)),
            dma((X - 1,)),
        ],
        compiler_params=pltpu.CompilerParams(collective_id=0, has_side_effects=True),
        name="adjoint",
    )(bias_exp, rsd_factor, slots, selection, galaxy_counts)
    grad_pos, grad_vel = pl.pallas_call(
        from_slots,
        out_shape=(
            jax.ShapeDtypeStruct(part_frac.shape, F32),
            jax.ShapeDtypeStruct((blocks, LANES), F32),
        ),
        in_specs=[smem, vmem],
        out_specs=(vmem, vmem),
        name="from_slots",
    )(place, pulled)
    return grad_pos, grad_vel.reshape(-1)


def solution(mesh):
    return jax.shard_map(
        on_device,
        mesh=mesh,
        in_specs=(
            P(None, ("los", "sky")),
            P(None, ("los", "sky")),
            P(("los", "sky")),
            P(("los", "sky")),
            P(("los", "sky")),
            P("los", "sky", None),
            P("los", "sky", None),
            P("los"),
            P("los"),
        ),
        out_specs=(P(None, ("los", "sky")), P(("los", "sky"))),
        check_vma=False,
    )
```

```python
import jax
import jax.numpy as jnp
from jax import lax
from jax.experimental import pallas as pl
from jax.experimental.pallas import tpu as pltpu
from jax.sharding import PartitionSpec as P

MESH = pl.DeviceIdType.MESH
F32 = jnp.float32
BF16 = jnp.bfloat16
LANES = 128
X = 4


def row_iota():
    return lax.broadcasted_iota(jnp.int32, (8, LANES), 0)


def split(values):
    high = values.astype(BF16)
    low = (values - high.astype(F32)).astype(BF16)
    return jnp.concatenate([high, low], axis=0)


def fetch(sources, targets, sems):
    copies = [
        pltpu.make_async_copy(source, target, sems.at[i])
        for i, (source, target) in enumerate(zip(sources, targets, strict=True))
    ]
    for copy in copies:
        copy.start()
    return copies


def to_slots(dest_in, counts_in, cell_in, frac_in, off_in, slots, place, *scratch):
    dest, counts, cell, frac, off, seen, sems = scratch
    copies = fetch(
        (dest_in, counts_in, cell_in, frac_in, off_in), (dest, counts, cell, frac, off), sems
    )
    sky_base = lax.axis_index("sky") * 4
    row = row_iota()
    empty = jnp.where(row == 0, -8.0, 0.0)
    for i in range(slots.shape[0]):
        slots[i] = empty
    for i in range(seen.shape[0]):
        seen[i] = 0
    for copy in copies:
        copy.wait()
    lane = lax.broadcasted_iota(jnp.int32, (1, LANES), 1)
    for b in range(dest.shape[0]):
        lanes = slice(b * LANES, (b + 1) * LANES)
        los = jnp.where(lane < counts[b], (cell[0:1, lanes] + off[b : b + 1, :]) & 3, -8)
        slab = dest[b]
        rank = seen[slab]
        seen[slab] = rank + 1
        slot = slab * 2 + rank
        place[b] = slot
        cells = jnp.concatenate([los, cell[1:2, lanes] - sky_base, cell[2:3, lanes]], axis=0)
        slots[slot, 0:3] = cells.astype(F32)
        slots[slot, 3:6] = frac[:, lanes]


def from_slots(place, pulled, out_pos, out_vel):
    for b in range(place.shape[0]):
        values = pulled[place[b]]
        out_pos[:, b * LANES : (b + 1) * LANES] = values[:3]
        out_vel[b : b + 1, :] = values[3:]


def slot_rows(slots, i):
    return [slots[i, r : r + 1] for r in range(6)]


def one_hot_deep(deep):
    iota = lax.broadcasted_iota(jnp.int32, (LANES, LANES), 0).astype(F32)
    return jnp.where(iota == deep, 1.0, 0.0).astype(BF16)


def kernel(
    bias_in,
    rsd_in,
    slots,
    selection_in,
    galaxies_in,
    pulled,
    bias,
    rsd,
    selection,
    galaxies,
    fetch_sems,
    hot,
    grid,
    grid_side,
    rx,
    rx_side,
    total,
    rz,
    field,
    field_side,
    rates,
    send_x,
    recv_x,
    send_side,
    recv_side,
    send_z,
    recv_z,
    send_cz,
    recv_cz,
    send_f,
    recv_f,
    send_fs,
    recv_fs,
    send_rz,
    recv_rz,
    send_rx,
    recv_rx,
):
    z_size = grid.shape[1]
    sky_size = lax.axis_size("sky")
    los_here = lax.axis_index("los")
    sky_here = lax.axis_index("sky")
    z_here = los_here // X
    x_here = los_here % X
    sky_up = (sky_here + 1) % sky_size
    sky_down = (sky_here + sky_size - 1) % sky_size

    def x_peer(k):
        return z_here * X + (x_here + k) % X

    def z_peer(k):
        return ((z_here + k) % z_size) * X + x_here

    barrier = pltpu.get_barrier_semaphore()
    for k in range(X):
        if k:
            pl.semaphore_signal(
                barrier, inc=1, device_id=(x_peer(k), sky_here), device_id_type=MESH
            )
        for sky_to in (sky_up, sky_down):
            pl.semaphore_signal(barrier, inc=1, device_id=(x_peer(k), sky_to), device_id_type=MESH)
    for k in range(1, z_size):
        pl.semaphore_signal(barrier, inc=1, device_id=(z_peer(k), sky_here), device_id_type=MESH)

    fetched = fetch(
        (bias_in, rsd_in, selection_in, galaxies_in), (bias, rsd, selection, galaxies), fetch_sems
    )
    row4 = lax.broadcasted_iota(jnp.int32, (4, LANES), 0)

    def by_row(scalars):
        value = jnp.full((4, LANES), scalars[3], F32)
        for i in (0, 1, 2):
            value = jnp.where(row4 == i, scalars[i], value)
        return value

    row = row_iota().astype(F32)

    def paint(t):
        tables, hots = [], []
        for slot in (0, 1):
            los, sky, deep, f_los, f_sky, f_deep = slot_rows(slots, t * 2 + slot)
            h_los = jnp.where(row == los, 1.0 - f_los, 0.0) + jnp.where(row == los + 1, f_los, 0.0)
            h_sky = jnp.where(row == sky, 1.0 - f_sky, 0.0) + jnp.where(row == sky + 1, f_sky, 0.0)
            lower, upper = h_los * (1.0 - f_deep), h_los * f_deep
            parts = []
            for s in range(5):
                parts += [h_sky[s : s + 1] * lower, h_sky[s : s + 1] * upper]
            tables.append(split(jnp.concatenate(parts, axis=0)))
            one_hot = one_hot_deep(deep)
            hot[t, :, slot * LANES : (slot + 1) * LANES] = one_hot
            hots.append(one_hot)
        result = lax.dot_general(
            jnp.concatenate(tables, axis=1),
            jnp.concatenate(hots, axis=1),
            (((1,), (1,)), ((), ())),
            preferred_element_type=F32,
        )
        result = result[:80] + result[80:]
        planes = []
        for s in range(5):
            lower, upper = result[s * 16 : s * 16 + 8], result[s * 16 + 8 : s * 16 + 16]
            planes.append(lower + pltpu.roll(upper, 1, 1))
        return planes

    order = [(z_size // 2 - 1 + j) % z_size for j in range(z_size)]

    def paint_step(step, previous):
        for i in range(2):
            j = step * 2 + i
            z = lax.rem(z_here + order[0] + j, z_size)
            for x in range(X):
                planes = paint(z * X + x)
                for s in range(5):
                    carried = jnp.where(row == 0, pltpu.roll(previous[s], 4, 0), 0.0)
                    whole = (planes[s] + carried)[:4]
                    if s < 4:
                        grid[x, j, s] = whole
                    else:
                        grid_side[x, j] = whole
                previous = planes
        return tuple(previous)

    zero = jnp.zeros((8, LANES), F32)
    before = lax.rem(z_here + order[-1], z_size)
    lax.fori_loop(0, z_size // 2, paint_step, tuple(paint(before * X + X - 1)))

    for copy in fetched:
        copy.wait()
    rates[x_here, z_here] = by_row(rsd)
    pl.semaphore_wait(barrier, 3 + 2 * X + z_size - 1)

    def remote(src, dst, send_sem, recv_sem, los_to, sky_to):
        return pltpu.make_async_remote_copy(
            src_ref=src,
            dst_ref=dst,
            send_sem=send_sem,
            recv_sem=recv_sem,
            device_id=(los_to, sky_to),
            device_id_type=MESH,
        )

    groups = [range(i, i + 2) for i in range(0, z_size, 2)]
    x_copies, side_copies, z_copies, rate_z = {}, {}, {}, {}
    for g, group in enumerate(groups):
        part = pl.ds(group[0], len(group))
        for k in (2, 1, 3, 0):
            x_to = (x_here + k) % X
            if k:
                x_copies[g, k] = remote(
                    grid.at[x_to, part],
                    rx.at[k - 1, part],
                    send_x.at[g, k - 1],
                    recv_x.at[g, k - 1],
                    x_peer(k),
                    sky_here,
                )
                x_copies[g, k].start()
            side_copies[g, k] = remote(
                grid_side.at[x_to, part],
                rx_side.at[k, part],
                send_side.at[g, k],
                recv_side.at[g, k],
                x_peer(k),
                sky_up,
            )
            side_copies[g, k].start()
    for k in range(1, z_size):
        rate_z[k] = remote(
            rates.at[x_here, z_here],
            rates.at[x_here, z_here],
            send_rz.at[k - 1],
            recv_rz.at[k - 1],
            z_peer(k),
            sky_here,
        )
        rate_z[k].start()

    for g, group in enumerate(groups):
        for k in range(X):
            if k:
                x_copies[g, k].wait_recv()
            side_copies[g, k].wait_recv()
        for j in group:
            for s in range(4):
                value = grid[x_here, j, s]
                for k in range(1, X):
                    value = value + rx[k - 1, j, s]
                if s == 0:
                    for k in range(X):
                        value = value + rx_side[k, j]
                total[j, s] = value
            k = order[j]
            if k:
                z_copies[k] = remote(
                    total.at[j],
                    rz.at[k - 1],
                    send_z.at[k - 1],
                    recv_z.at[k - 1],
                    z_peer(k),
                    sky_here,
                )
                z_copies[k].start()

    for k in range(1, z_size):
        rate_z[k].wait_recv()
    rate_x = {}
    for k in range(1, X):
        rate_x[k] = remote(
            rates.at[x_here],
            rates.at[x_here],
            send_rx.at[k - 1],
            recv_rx.at[k - 1],
            x_peer(k),
            sky_here,
        )
        rate_x[k].start()

    exponent = by_row(bias)
    for k in range(1, z_size):
        z_copies[k].wait_recv()
    for s in range(4):
        density = total[order.index(0), s]
        for k in range(1, z_size):
            density = density + rz[k - 1, s]
        mean = jnp.concatenate([selection[l, s : s + 1] for l in range(4)], axis=0)
        seen = jnp.concatenate([galaxies[l, s : s + 1] for l in range(4)], axis=0).astype(F32)
        shifted = density + 0.5
        intensity = mean * jnp.exp(exponent * jnp.log(shifted))
        field[x_here, z_here, s] = (1.0 - seen / intensity) * exponent * intensity / shifted

    cz_copies = {}
    for k in sorted(range(1, z_size), key=lambda k: -min(k, z_size - k)):
        cz_copies[k] = remote(
            field.at[x_here, z_here],
            field.at[x_here, z_here],
            send_cz.at[k - 1],
            recv_cz.at[k - 1],
            z_peer(k),
            sky_here,
        )
        cz_copies[k].start()
    f_copies, fs_copies = {}, {}
    for j in sorted(range(z_size), key=lambda k: min(k, z_size - k)):
        if j:
            cz_copies[j].wait_recv()
        z_from = (z_here + z_size - j) % z_size
        for k in (2, 1, 3, 0):
            if k:
                f_copies[j, k] = remote(
                    field.at[x_here, z_from],
                    field.at[x_here, z_from],
                    send_f.at[j, k - 1],
                    recv_f.at[j, k - 1],
                    x_peer(k),
                    sky_here,
                )
                f_copies[j, k].start()
            fs_copies[j, k] = remote(
                field.at[x_here, z_from, 0],
                field_side.at[x_here, z_from],
                send_fs.at[j, k],
                recv_fs.at[j, k],
                x_peer(k),
                sky_down,
            )
            fs_copies[j, k].start()
    for k in range(1, X):
        rate_x[k].wait_recv()
    def pull(z, x):
        t = z * X + x
        z_next, x_next = (z, x + 1) if x + 1 < X else ((z + 1) % z_size, 0)
        rows = []
        for s in range(5):
            if s < 4:
                value = jnp.concatenate([field[x, z, s], field[x_next, z_next, s]], axis=0)
            else:
                value = jnp.concatenate([field_side[x, z], field_side[x_next, z_next]], axis=0)
            rows += [value, pltpu.roll(value, LANES - 1, 1)]
        picked = jnp.dot(
            split(jnp.concatenate(rows, axis=0)), hot[t], preferred_element_type=F32
        )
        picked = picked[:80] + picked[80:]
        rate = jnp.concatenate([rates[x, z], jnp.zeros((4, LANES), F32)], axis=0)
        for slot in (0, 1):
            los, sky, deep, f_los, f_sky, f_deep = slot_rows(slots, t * 2 + slot)
            at, above = row == los, row == los + 1
            h_los = jnp.where(at, 1.0 - f_los, 0.0) + jnp.where(above, f_los, 0.0)
            d_los = jnp.where(above, 1.0, 0.0) - jnp.where(at, 1.0, 0.0)
            r_los = jnp.where(at, rate, 0.0)
            at, above = row == sky, row == sky + 1
            h_sky = jnp.where(at, 1.0 - f_sky, 0.0) + jnp.where(above, f_sky, 0.0)
            d_sky = jnp.where(above, 1.0, 0.0) - jnp.where(at, 1.0, 0.0)
            lanes = slice(slot * LANES, (slot + 1) * LANES)
            val, val_sky, val_deep = zero, zero, zero
            for s in range(5):
                here = picked[s * 16 : s * 16 + 8, lanes]
                step = picked[s * 16 + 8 : s * 16 + 16, lanes] - here
                mixed = here + f_deep * step
                val = val + h_sky[s : s + 1] * mixed
                val_sky = val_sky + d_sky[s : s + 1] * mixed
                val_deep = val_deep + h_sky[s : s + 1] * step
            g_los = jnp.sum(d_los * val, axis=0, keepdims=True)
            g_sky = jnp.sum(h_los * val_sky, axis=0, keepdims=True)
            g_deep = jnp.sum(h_los * val_deep, axis=0, keepdims=True)
            speed = jnp.sum(r_los, axis=0, keepdims=True) * g_los
            pulled[t * 2 + slot] = jnp.concatenate([g_los, g_sky, g_deep, speed], axis=0)

    waited = set()
    for g in range(z_size // 2):
        for j in (0, g + 1, z_size - g - 1):
            if j not in waited:
                waited.add(j)
                for k in range(X):
                    if k:
                        f_copies[j, k].wait_recv()
                    fs_copies[j, k].wait_recv()
        for z in ((z_here + z_size - g - 1) % z_size, (z_here + g) % z_size):
            for x in range(X):
                pull(z, x)

    for copies in (
        x_copies,
        side_copies,
        rate_z,
        z_copies,
        rate_x,
        cz_copies,
        f_copies,
        fs_copies,
    ):
        for copy in copies.values():
            copy.wait_send()


def on_device(
    part_cell,
    part_frac,
    los_offset,
    block_dest,
    block_count,
    selection,
    galaxy_counts,
    bias_exp,
    rsd_factor,
):
    los_size = lax.axis_size("los")
    z_size = los_size // X
    blocks = block_dest.shape[0]
    vmem = pl.BlockSpec(memory_space=pltpu.VMEM)
    smem = pl.BlockSpec(memory_space=pltpu.SMEM)
    hbm = pl.BlockSpec(memory_space=pltpu.HBM)
    dma = pltpu.SemaphoreType.DMA
    slots, place = pl.pallas_call(
        to_slots,
        out_shape=(
            jax.ShapeDtypeStruct((2 * los_size, 8, LANES), F32),
            jax.ShapeDtypeStruct((blocks,), jnp.int32),
        ),
        in_specs=[hbm] * 5,
        out_specs=(vmem, smem),
        scratch_shapes=[
            pltpu.SMEM((blocks,), jnp.int32),
            pltpu.SMEM((blocks,), jnp.int32),
            pltpu.VMEM(part_cell.shape, jnp.int32),
            pltpu.VMEM(part_frac.shape, F32),
            pltpu.VMEM((blocks, LANES), jnp.int32),
            pltpu.SMEM((los_size,), jnp.int32),
            dma((5,)),
        ],
        name="to_slots",
    )(block_dest, block_count, part_cell, part_frac, los_offset.reshape(blocks, LANES))
    pulled = pl.pallas_call(
        kernel,
        out_shape=jax.ShapeDtypeStruct((2 * los_size, 4, LANES), F32),
        in_specs=[hbm, hbm, vmem, hbm, hbm],
        out_specs=vmem,
        scratch_shapes=[
            pltpu.SMEM(bias_exp.shape, F32),
            pltpu.SMEM(rsd_factor.shape, F32),
            pltpu.VMEM(selection.shape, F32),
            pltpu.VMEM(galaxy_counts.shape, jnp.int32),
            dma((4,)),
            pltpu.VMEM((los_size, LANES, 2 * LANES), BF16),
            pltpu.VMEM((X, z_size, 4, 4, LANES), F32),
            pltpu.VMEM((X, z_size, 4, LANES), F32),
            pltpu.VMEM((X - 1, z_size, 4, 4, LANES), F32),
            pltpu.VMEM((X, z_size, 4, LANES), F32),
            pltpu.VMEM((z_size, 4, 4, LANES), F32),
            pltpu.VMEM((z_size - 1, 4, 4, LANES), F32),
            pltpu.VMEM((X, z_size, 4, 4, LANES), F32),
            pltpu.VMEM((X, z_size, 4, LANES), F32),
            pltpu.VMEM((X, z_size, 4, LANES), F32),
            dma((z_size // 2, X - 1)),
            dma((z_size // 2, X - 1)),
            dma((z_size // 2, X)),
            dma((z_size // 2, X)),
            dma((z_size - 1,)),
            dma((z_size - 1,)),
            dma((z_size - 1,)),
            dma((z_size - 1,)),
            dma((z_size, X - 1)),
            dma((z_size, X - 1)),
            dma((z_size, X)),
            dma((z_size, X)),
            dma((z_size - 1,)),
            dma((z_size - 1,)),
            dma((X - 1,)),
            dma((X - 1,)),
        ],
        compiler_params=pltpu.CompilerParams(
            collective_id=0, has_side_effects=True
        ),
        name="adjoint",
    )(bias_exp, rsd_factor, slots, selection, galaxy_counts)
    grad_pos, grad_vel = pl.pallas_call(
        from_slots,
        out_shape=(
            jax.ShapeDtypeStruct(part_frac.shape, F32),
            jax.ShapeDtypeStruct((blocks, LANES), F32),
        ),
        in_specs=[smem, vmem],
        out_specs=(vmem, vmem),
        name="from_slots",
    )(place, pulled)
    return grad_pos, grad_vel.reshape(-1)


def solution(mesh):
    return jax.shard_map(
        on_device,
        mesh=mesh,
        in_specs=(
            P(None, ("los", "sky")),
            P(None, ("los", "sky")),
            P(("los", "sky")),
            P(("los", "sky")),
            P(("los", "sky")),
            P("los", "sky", None),
            P("los", "sky", None),
            P("los"),
            P("los"),
        ),
        out_specs=(P(None, ("los", "sky")), P(("los", "sky"))),
        check_vma=False,
    )
```

```python
import jax
import jax.numpy as jnp
from jax import lax
from jax.experimental import pallas as pl
from jax.experimental.pallas import tpu as pltpu
from jax.sharding import PartitionSpec as P

MESH = pl.DeviceIdType.MESH
F32 = jnp.float32
BF16 = jnp.bfloat16
LANES = 128
X = 4


def row_iota():
    return lax.broadcasted_iota(jnp.int32, (8, LANES), 0)


def split(values):
    high = values.astype(BF16)
    low = (values - high.astype(F32)).astype(BF16)
    return jnp.concatenate([high, low], axis=0)


def fetch(sources, targets, sems):
    copies = [
        pltpu.make_async_copy(source, target, sems.at[i])
        for i, (source, target) in enumerate(zip(sources, targets, strict=True))
    ]
    for copy in copies:
        copy.start()
    return copies


def thirds(values):
    high = values.astype(BF16)
    rest = values - high.astype(F32)
    middle = rest.astype(BF16)
    return [high, middle, (rest - middle.astype(F32)).astype(BF16)]


def slot_matrix(dest, counts, los_size):
    shape = (los_size, dest.shape[1])
    slab = lax.broadcasted_iota(jnp.int32, shape, 0)
    code = lax.broadcasted_iota(jnp.int32, shape, 1) * 256 + counts[...]
    code = jnp.where(slab == dest[...], code, -1).astype(F32)
    most = jnp.max(code, axis=1, keepdims=True)
    least = jnp.min(jnp.where(code < 0.0, 65536.0, code), axis=1, keepdims=True)
    single = least >= most
    first = jnp.where(code == least, 1.0, 0.0)
    second = jnp.where(single, 0.0, jnp.where(code == most, 1.0, 0.0))
    matrix = jnp.concatenate([first, second], axis=0)
    live = jnp.concatenate([jnp.maximum(least, 0.0), most], axis=0).astype(jnp.int32) & 255
    some = jnp.concatenate([most >= 0.0, jnp.logical_not(single)], axis=0)
    return matrix, jnp.where(some, live, 0)


def slot_rows(slots, slot, t):
    return [slots[slot, r, pl.ds(t, 1), :] for r in range(6)]


def one_hot_deep(deep):
    iota = lax.broadcasted_iota(jnp.int32, (LANES, LANES), 0).astype(F32)
    return jnp.where(iota == deep, 1.0, 0.0).astype(BF16)


def kernel(
    dest_in,
    counts_in,
    cell_in,
    frac_in,
    off_in,
    bias_in,
    rsd_in,
    selection_in,
    galaxies_in,
    out_pos,
    out_vel,
    dest,
    counts,
    cell,
    frac,
    off,
    bias,
    rsd,
    selection,
    galaxies,
    fetch_sems,
    rows_in,
    slots,
    pulled,
    hot,
    grid,
    grid_side,
    rx,
    rx_side,
    total,
    rz,
    field,
    field_side,
    rates,
    send_x,
    recv_x,
    send_side,
    recv_side,
    send_z,
    recv_z,
    send_cz,
    recv_cz,
    send_f,
    recv_f,
    send_fs,
    recv_fs,
    send_rz,
    recv_rz,
    send_rx,
    recv_rx,
):
    z_size = grid.shape[1]
    sky_size = lax.axis_size("sky")
    los_size = X * z_size
    los_here = lax.axis_index("los")
    sky_here = lax.axis_index("sky")
    z_here = los_here // X
    x_here = los_here % X
    sky_up = (sky_here + 1) % sky_size
    sky_down = (sky_here + sky_size - 1) % sky_size

    def x_peer(k):
        return z_here * X + (x_here + k) % X

    def z_peer(k):
        return ((z_here + k) % z_size) * X + x_here

    barrier = pltpu.get_barrier_semaphore()
    for k in range(X):
        if k:
            pl.semaphore_signal(
                barrier, inc=1, device_id=(x_peer(k), sky_here), device_id_type=MESH
            )
        for sky_to in (sky_up, sky_down):
            pl.semaphore_signal(barrier, inc=1, device_id=(x_peer(k), sky_to), device_id_type=MESH)
    for k in range(1, z_size):
        pl.semaphore_signal(barrier, inc=1, device_id=(z_peer(k), sky_here), device_id_type=MESH)

    fetched = fetch(
        (
            dest_in,
            counts_in,
            cell_in,
            frac_in,
            off_in,
            bias_in,
            rsd_in,
            selection_in,
            galaxies_in,
        ),
        (dest, counts, cell, frac, off, bias, rsd, selection, galaxies),
        fetch_sems,
    )
    row4 = lax.broadcasted_iota(jnp.int32, (4, LANES), 0)

    def by_row(scalars):
        value = jnp.full((4, LANES), scalars[3], F32)
        for i in (0, 1, 2):
            value = jnp.where(row4 == i, scalars[i], value)
        return value

    row = row_iota().astype(F32)

    for copy in fetched[:5]:
        copy.wait()
    blocks = dest.shape[1]
    matrix, live = slot_matrix(dest, counts, los_size)
    for b in range(blocks):
        lanes = slice(b * LANES, (b + 1) * LANES)
        cells = cell[:, lanes].astype(F32)
        fracs = frac[:, lanes]
        for r in range(3):
            rows_in[r, b : b + 1, :] = cells[r : r + 1]
            rows_in[3 + r, b : b + 1, :] = fracs[r : r + 1]
    los_row = ((rows_in[0].astype(jnp.int32) + off[...]) & 3).astype(F32)
    sky_row = rows_in[1] - (sky_here * 4).astype(F32)
    parts = [los_row.astype(BF16), sky_row.astype(BF16), rows_in[2].astype(BF16)]
    for r in range(3):
        parts += thirds(rows_in[3 + r])
    placed = jnp.dot(
        matrix.astype(BF16), jnp.concatenate(parts, axis=1), preferred_element_type=F32
    )
    lane = lax.broadcasted_iota(jnp.int32, (2 * los_size, LANES), 1)
    for r in range(6):
        part = [placed[:, i * LANES : (i + 1) * LANES] for i in range(12)]
        if r < 3:
            value = jnp.where(lane < live, part[0], -8.0) if r == 0 else part[r]
        else:
            value = (part[3 * r - 6] + part[3 * r - 5]) + part[3 * r - 4]
        for slot in (0, 1):
            slots[slot, r] = value[slot * los_size : (slot + 1) * los_size]

    def paint(t):
        tables, hots = [], []
        for slot in (0, 1):
            los, sky, deep, f_los, f_sky, f_deep = slot_rows(slots, slot, t)
            h_los = jnp.where(row == los, 1.0 - f_los, 0.0) + jnp.where(row == los + 1, f_los, 0.0)
            h_sky = jnp.where(row == sky, 1.0 - f_sky, 0.0) + jnp.where(row == sky + 1, f_sky, 0.0)
            lower, upper = h_los * (1.0 - f_deep), h_los * f_deep
            parts = []
            for s in range(5):
                parts += [h_sky[s : s + 1] * lower, h_sky[s : s + 1] * upper]
            tables.append(split(jnp.concatenate(parts, axis=0)))
            one_hot = one_hot_deep(deep)
            hot[t, :, slot * LANES : (slot + 1) * LANES] = one_hot
            hots.append(one_hot)
        result = lax.dot_general(
            jnp.concatenate(tables, axis=1),
            jnp.concatenate(hots, axis=1),
            (((1,), (1,)), ((), ())),
            preferred_element_type=F32,
        )
        result = result[:80] + result[80:]
        planes = []
        for s in range(5):
            lower, upper = result[s * 16 : s * 16 + 8], result[s * 16 + 8 : s * 16 + 16]
            planes.append(lower + pltpu.roll(upper, 1, 1))
        return planes

    order = [(z_size // 2 - 1 + j) % z_size for j in range(z_size)]

    def paint_step(step, previous):
        for i in range(2):
            j = step * 2 + i
            z = lax.rem(z_here + order[0] + j, z_size)
            for x in range(X):
                planes = paint(z * X + x)
                for s in range(5):
                    carried = jnp.where(row == 0, pltpu.roll(previous[s], 4, 0), 0.0)
                    whole = (planes[s] + carried)[:4]
                    if s < 4:
                        grid[x, j, s] = whole
                    else:
                        grid_side[x, j] = whole
                previous = planes
        return tuple(previous)

    zero = jnp.zeros((8, LANES), F32)
    before = lax.rem(z_here + order[-1], z_size)
    lax.fori_loop(0, z_size // 2, paint_step, tuple(paint(before * X + X - 1)))

    for copy in fetched[5:]:
        copy.wait()
    rates[x_here, z_here] = by_row(rsd)
    pl.semaphore_wait(barrier, 3 + 2 * X + z_size - 1)

    def remote(src, dst, send_sem, recv_sem, los_to, sky_to):
        return pltpu.make_async_remote_copy(
            src_ref=src,
            dst_ref=dst,
            send_sem=send_sem,
            recv_sem=recv_sem,
            device_id=(los_to, sky_to),
            device_id_type=MESH,
        )

    groups = [range(i, i + 2) for i in range(0, z_size, 2)]
    x_copies, side_copies, z_copies, rate_z = {}, {}, {}, {}
    for g, group in enumerate(groups):
        part = pl.ds(group[0], len(group))
        for k in (2, 1, 3, 0):
            x_to = (x_here + k) % X
            if k:
                x_copies[g, k] = remote(
                    grid.at[x_to, part],
                    rx.at[k - 1, part],
                    send_x.at[g, k - 1],
                    recv_x.at[g, k - 1],
                    x_peer(k),
                    sky_here,
                )
                x_copies[g, k].start()
            side_copies[g, k] = remote(
                grid_side.at[x_to, part],
                rx_side.at[k, part],
                send_side.at[g, k],
                recv_side.at[g, k],
                x_peer(k),
                sky_up,
            )
            side_copies[g, k].start()
    for k in range(1, z_size):
        rate_z[k] = remote(
            rates.at[x_here, z_here],
            rates.at[x_here, z_here],
            send_rz.at[k - 1],
            recv_rz.at[k - 1],
            z_peer(k),
            sky_here,
        )
        rate_z[k].start()

    for g, group in enumerate(groups):
        for k in range(X):
            if k:
                x_copies[g, k].wait_recv()
            side_copies[g, k].wait_recv()
        for j in group:
            for s in range(4):
                value = grid[x_here, j, s]
                for k in range(1, X):
                    value = value + rx[k - 1, j, s]
                if s == 0:
                    for k in range(X):
                        value = value + rx_side[k, j]
                total[j, s] = value
            k = order[j]
            if k:
                z_copies[k] = remote(
                    total.at[j],
                    rz.at[k - 1],
                    send_z.at[k - 1],
                    recv_z.at[k - 1],
                    z_peer(k),
                    sky_here,
                )
                z_copies[k].start()

    for k in range(1, z_size):
        rate_z[k].wait_recv()
    rate_x = {}
    for k in range(1, X):
        rate_x[k] = remote(
            rates.at[x_here],
            rates.at[x_here],
            send_rx.at[k - 1],
            recv_rx.at[k - 1],
            x_peer(k),
            sky_here,
        )
        rate_x[k].start()

    exponent = by_row(bias)
    for k in range(1, z_size):
        z_copies[k].wait_recv()
    for s in range(4):
        density = total[order.index(0), s]
        for k in range(1, z_size):
            density = density + rz[k - 1, s]
        mean = jnp.concatenate([selection[l, s : s + 1] for l in range(4)], axis=0)
        seen = jnp.concatenate([galaxies[l, s : s + 1] for l in range(4)], axis=0).astype(F32)
        shifted = density + 0.5
        intensity = mean * jnp.exp(exponent * jnp.log(shifted))
        field[x_here, z_here, s] = (1.0 - seen / intensity) * exponent * intensity / shifted

    cz_copies = {}
    for k in sorted(range(1, z_size), key=lambda k: -min(k, z_size - k)):
        cz_copies[k] = remote(
            field.at[x_here, z_here],
            field.at[x_here, z_here],
            send_cz.at[k - 1],
            recv_cz.at[k - 1],
            z_peer(k),
            sky_here,
        )
        cz_copies[k].start()
    f_copies, fs_copies = {}, {}
    for j in sorted(range(z_size), key=lambda k: min(k, z_size - k)):
        if j:
            cz_copies[j].wait_recv()
        z_from = (z_here + z_size - j) % z_size
        for k in (2, 1, 3, 0):
            if k:
                f_copies[j, k] = remote(
                    field.at[x_here, z_from],
                    field.at[x_here, z_from],
                    send_f.at[j, k - 1],
                    recv_f.at[j, k - 1],
                    x_peer(k),
                    sky_here,
                )
                f_copies[j, k].start()
            fs_copies[j, k] = remote(
                field.at[x_here, z_from, 0],
                field_side.at[x_here, z_from],
                send_fs.at[j, k],
                recv_fs.at[j, k],
                x_peer(k),
                sky_down,
            )
            fs_copies[j, k].start()
    for k in range(1, X):
        rate_x[k].wait_recv()
    def pull(z, x):
        t = z * X + x
        z_next, x_next = (z, x + 1) if x + 1 < X else ((z + 1) % z_size, 0)
        rows = []
        for s in range(5):
            if s < 4:
                value = jnp.concatenate([field[x, z, s], field[x_next, z_next, s]], axis=0)
            else:
                value = jnp.concatenate([field_side[x, z], field_side[x_next, z_next]], axis=0)
            rows += [value, pltpu.roll(value, LANES - 1, 1)]
        picked = jnp.dot(
            split(jnp.concatenate(rows, axis=0)), hot[t], preferred_element_type=F32
        )
        picked = picked[:80] + picked[80:]
        rate = jnp.concatenate([rates[x, z], jnp.zeros((4, LANES), F32)], axis=0)
        for slot in (0, 1):
            los, sky, deep, f_los, f_sky, f_deep = slot_rows(slots, slot, t)
            at, above = row == los, row == los + 1
            h_los = jnp.where(at, 1.0 - f_los, 0.0) + jnp.where(above, f_los, 0.0)
            d_los = jnp.where(above, 1.0, 0.0) - jnp.where(at, 1.0, 0.0)
            r_los = jnp.where(at, rate, 0.0)
            at, above = row == sky, row == sky + 1
            h_sky = jnp.where(at, 1.0 - f_sky, 0.0) + jnp.where(above, f_sky, 0.0)
            d_sky = jnp.where(above, 1.0, 0.0) - jnp.where(at, 1.0, 0.0)
            lanes = slice(slot * LANES, (slot + 1) * LANES)
            val, val_sky, val_deep = zero, zero, zero
            for s in range(5):
                here = picked[s * 16 : s * 16 + 8, lanes]
                step = picked[s * 16 + 8 : s * 16 + 16, lanes] - here
                mixed = here + f_deep * step
                val = val + h_sky[s : s + 1] * mixed
                val_sky = val_sky + d_sky[s : s + 1] * mixed
                val_deep = val_deep + h_sky[s : s + 1] * step
            g_los = jnp.sum(d_los * val, axis=0, keepdims=True)
            g_sky = jnp.sum(h_los * val_sky, axis=0, keepdims=True)
            g_deep = jnp.sum(h_los * val_deep, axis=0, keepdims=True)
            speed = jnp.sum(r_los, axis=0, keepdims=True) * g_los
            for r, value in enumerate((g_los, g_sky, g_deep, speed)):
                pulled[slot, r, pl.ds(t, 1), :] = value

    waited = set()
    for g in range(z_size // 2):
        for j in (0, g + 1, z_size - g - 1):
            if j not in waited:
                waited.add(j)
                for k in range(X):
                    if k:
                        f_copies[j, k].wait_recv()
                    fs_copies[j, k].wait_recv()
        for z in ((z_here + z_size - g - 1) % z_size, (z_here + g) % z_size):
            for x in range(X):
                pull(z, x)

    back = jnp.transpose(matrix).astype(BF16)
    parts = []
    for slot in (0, 1):
        parts.append(jnp.concatenate([pulled[slot, r] for r in range(4)], axis=1))
    result = jnp.dot(
        jnp.concatenate([back] * 3, axis=1),
        jnp.concatenate(thirds(jnp.concatenate(parts, axis=0)), axis=0),
        preferred_element_type=F32,
    )
    for r in range(3):
        out_pos[r] = result[:, r * LANES : (r + 1) * LANES]
    out_vel[...] = result[:, 3 * LANES :]

    for copies in (
        x_copies,
        side_copies,
        rate_z,
        z_copies,
        rate_x,
        cz_copies,
        f_copies,
        fs_copies,
    ):
        for copy in copies.values():
            copy.wait_send()


def on_device(
    part_cell,
    part_frac,
    los_offset,
    block_dest,
    block_count,
    selection,
    galaxy_counts,
    bias_exp,
    rsd_factor,
):
    los_size = lax.axis_size("los")
    z_size = los_size // X
    blocks = block_dest.shape[0]
    vmem = pl.BlockSpec(memory_space=pltpu.VMEM)
    hbm = pl.BlockSpec(memory_space=pltpu.HBM)
    dma = pltpu.SemaphoreType.DMA
    inputs = (
        block_dest.reshape(1, blocks),
        block_count.reshape(1, blocks),
        part_cell,
        part_frac,
        los_offset.reshape(blocks, LANES),
        bias_exp,
        rsd_factor,
        selection,
        galaxy_counts,
    )
    grad_pos, grad_vel = pl.pallas_call(
        kernel,
        out_shape=(
            jax.ShapeDtypeStruct((3, blocks, LANES), F32),
            jax.ShapeDtypeStruct((blocks, LANES), F32),
        ),
        in_specs=[hbm] * len(inputs),
        out_specs=(vmem, vmem),
        scratch_shapes=[
            *[
                (pltpu.SMEM if value.ndim == 1 else pltpu.VMEM)(value.shape, value.dtype)
                for value in inputs
            ],
            dma((len(inputs),)),
            pltpu.VMEM((6, blocks, LANES), F32),
            pltpu.VMEM((2, 6, los_size, LANES), F32),
            pltpu.VMEM((2, 4, los_size, LANES), F32),
            pltpu.VMEM((los_size, LANES, 2 * LANES), BF16),
            pltpu.VMEM((X, z_size, 4, 4, LANES), F32),
            pltpu.VMEM((X, z_size, 4, LANES), F32),
            pltpu.VMEM((X - 1, z_size, 4, 4, LANES), F32),
            pltpu.VMEM((X, z_size, 4, LANES), F32),
            pltpu.VMEM((z_size, 4, 4, LANES), F32),
            pltpu.VMEM((z_size - 1, 4, 4, LANES), F32),
            pltpu.VMEM((X, z_size, 4, 4, LANES), F32),
            pltpu.VMEM((X, z_size, 4, LANES), F32),
            pltpu.VMEM((X, z_size, 4, LANES), F32),
            dma((z_size // 2, X - 1)),
            dma((z_size // 2, X - 1)),
            dma((z_size // 2, X)),
            dma((z_size // 2, X)),
            dma((z_size - 1,)),
            dma((z_size - 1,)),
            dma((z_size - 1,)),
            dma((z_size - 1,)),
            dma((z_size, X - 1)),
            dma((z_size, X - 1)),
            dma((z_size, X)),
            dma((z_size, X)),
            dma((z_size - 1,)),
            dma((z_size - 1,)),
            dma((X - 1,)),
            dma((X - 1,)),
        ],
        compiler_params=pltpu.CompilerParams(
            collective_id=0, has_side_effects=True
        ),
        name="adjoint",
    )(*inputs)
    return grad_pos.reshape(3, -1), grad_vel.reshape(-1)


def solution(mesh):
    return jax.shard_map(
        on_device,
        mesh=mesh,
        in_specs=(
            P(None, ("los", "sky")),
            P(None, ("los", "sky")),
            P(("los", "sky")),
            P(("los", "sky")),
            P(("los", "sky")),
            P("los", "sky", None),
            P("los", "sky", None),
            P("los"),
            P("los"),
        ),
        out_specs=(P(None, ("los", "sky")), P(("los", "sky"))),
        check_vma=False,
    )
```

```python
import jax
import jax.numpy as jnp
from jax import lax
from jax.experimental import pallas as pl
from jax.experimental.pallas import tpu as pltpu
from jax.sharding import PartitionSpec as P

MESH = pl.DeviceIdType.MESH
F32 = jnp.float32
BF16 = jnp.bfloat16
LANES = 128
X = 4


def row_iota():
    return lax.broadcasted_iota(jnp.int32, (8, LANES), 0)


def split(values):
    high = values.astype(BF16)
    low = (values - high.astype(F32)).astype(BF16)
    return jnp.concatenate([high, low], axis=0)


def fetch(sources, targets, sems):
    copies = [
        pltpu.make_async_copy(source, target, sems.at[i])
        for i, (source, target) in enumerate(zip(sources, targets, strict=True))
    ]
    for copy in copies:
        copy.start()
    return copies


def thirds(values):
    high = values.astype(BF16)
    rest = values - high.astype(F32)
    middle = rest.astype(BF16)
    return [high, middle, (rest - middle.astype(F32)).astype(BF16)]


def slot_matrix(dest, counts, los_size):
    shape = (los_size, dest.shape[1])
    slab = lax.broadcasted_iota(jnp.int32, shape, 0)
    code = lax.broadcasted_iota(jnp.int32, shape, 1) * 256 + counts[...]
    code = jnp.where(slab == dest[...], code, -1).astype(F32)
    most = jnp.max(code, axis=1, keepdims=True)
    least = jnp.min(jnp.where(code < 0.0, 65536.0, code), axis=1, keepdims=True)
    single = least >= most
    first = jnp.where(code == least, 1.0, 0.0)
    second = jnp.where(single, 0.0, jnp.where(code == most, 1.0, 0.0))
    matrix = jnp.concatenate([first, second], axis=0)
    live = jnp.concatenate([jnp.maximum(least, 0.0), most], axis=0).astype(jnp.int32) & 255
    some = jnp.concatenate([most >= 0.0, jnp.logical_not(single)], axis=0)
    return matrix, jnp.where(some, live, 0)


def slot_rows(slots, slot, t):
    return [slots[slot, r, pl.ds(t, 1), :] for r in range(6)]


def one_hot_deep(deep):
    iota = lax.broadcasted_iota(jnp.int32, (LANES, LANES), 0).astype(F32)
    return jnp.where(iota == deep, 1.0, 0.0).astype(BF16)


def kernel(
    dest_in,
    counts_in,
    cell_in,
    frac_in,
    off_in,
    bias_in,
    rsd_in,
    selection_in,
    galaxies_in,
    out_pos,
    out_vel,
    dest,
    counts,
    cell,
    frac,
    off,
    bias,
    rsd,
    selection,
    galaxies,
    fetch_sems,
    rows_in,
    slots,
    pulled,
    hot,
    grid,
    grid_side,
    rx,
    rx_side,
    total,
    rz,
    field,
    field_side,
    rates,
    send_sems,
    recv_x,
    recv_z,
    recv_cz,
    recv_f,
    recv_rates,
):
    z_size = grid.shape[1]
    sky_size = lax.axis_size("sky")
    los_size = X * z_size
    los_here = lax.axis_index("los")
    sky_here = lax.axis_index("sky")
    z_here = los_here // X
    x_here = los_here % X
    sky_up = (sky_here + 1) % sky_size
    sky_down = (sky_here + sky_size - 1) % sky_size

    def x_peer(k):
        return z_here * X + (x_here + k) % X

    def z_peer(k):
        return ((z_here + k) % z_size) * X + x_here

    fetched = fetch(
        (
            dest_in,
            counts_in,
            cell_in,
            frac_in,
            off_in,
            bias_in,
            rsd_in,
            selection_in,
            galaxies_in,
        ),
        (dest, counts, cell, frac, off, bias, rsd, selection, galaxies),
        fetch_sems,
    )
    barrier = pltpu.get_barrier_semaphore()
    for k in range(X):
        if k:
            pl.semaphore_signal(
                barrier, inc=1, device_id=(x_peer(k), sky_here), device_id_type=MESH
            )
        for sky_to in (sky_up, sky_down):
            pl.semaphore_signal(barrier, inc=1, device_id=(x_peer(k), sky_to), device_id_type=MESH)
    for k in range(1, z_size):
        pl.semaphore_signal(barrier, inc=1, device_id=(z_peer(k), sky_here), device_id_type=MESH)

    row4 = lax.broadcasted_iota(jnp.int32, (4, LANES), 0)

    def by_row(scalars):
        value = jnp.full((4, LANES), scalars[3], F32)
        for i in (0, 1, 2):
            value = jnp.where(row4 == i, scalars[i], value)
        return value

    row = row_iota().astype(F32)

    for copy in fetched[:5]:
        copy.wait()
    blocks = dest.shape[1]
    matrix, live = slot_matrix(dest, counts, los_size)
    for b in range(blocks):
        lanes = slice(b * LANES, (b + 1) * LANES)
        cells = cell[:, lanes].astype(F32)
        fracs = frac[:, lanes]
        for r in range(3):
            rows_in[r, b : b + 1, :] = cells[r : r + 1]
            rows_in[3 + r, b : b + 1, :] = fracs[r : r + 1]
    los_row = ((rows_in[0].astype(jnp.int32) + off[...]) & 3).astype(F32)
    sky_row = rows_in[1] - (sky_here * 4).astype(F32)
    parts = [los_row.astype(BF16), sky_row.astype(BF16), rows_in[2].astype(BF16)]
    for r in range(3):
        parts += thirds(rows_in[3 + r])
    placed = jnp.dot(
        matrix.astype(BF16), jnp.concatenate(parts, axis=1), preferred_element_type=F32
    )
    lane = lax.broadcasted_iota(jnp.int32, (2 * los_size, LANES), 1)
    for r in range(6):
        part = [placed[:, i * LANES : (i + 1) * LANES] for i in range(12)]
        if r < 3:
            value = jnp.where(lane < live, part[0], -8.0) if r == 0 else part[r]
        else:
            value = (part[3 * r - 6] + part[3 * r - 5]) + part[3 * r - 4]
        for slot in (0, 1):
            slots[slot, r] = value[slot * los_size : (slot + 1) * los_size]

    def paint(t):
        tables, hots = [], []
        for slot in (0, 1):
            los, sky, deep, f_los, f_sky, f_deep = slot_rows(slots, slot, t)
            h_los = jnp.where(row == los, 1.0 - f_los, 0.0) + jnp.where(row == los + 1, f_los, 0.0)
            h_sky = jnp.where(row == sky, 1.0 - f_sky, 0.0) + jnp.where(row == sky + 1, f_sky, 0.0)
            lower, upper = h_los * (1.0 - f_deep), h_los * f_deep
            parts = []
            for s in range(5):
                parts += [h_sky[s : s + 1] * lower, h_sky[s : s + 1] * upper]
            tables.append(split(jnp.concatenate(parts, axis=0)))
            one_hot = one_hot_deep(deep)
            hot[t, :, slot * LANES : (slot + 1) * LANES] = one_hot
            hots.append(one_hot)
        result = lax.dot_general(
            jnp.concatenate(tables, axis=1),
            jnp.concatenate(hots, axis=1),
            (((1,), (1,)), ((), ())),
            preferred_element_type=F32,
        )
        result = result[:80] + result[80:]
        planes = []
        for s in range(5):
            lower, upper = result[s * 16 : s * 16 + 8], result[s * 16 + 8 : s * 16 + 16]
            planes.append(lower + pltpu.roll(upper, 1, 1))
        return planes

    order = [(z_size // 2 - 1 + j) % z_size for j in range(z_size)]

    def remote(src, dst, send_sem, recv_sem, los_to, sky_to):
        return pltpu.make_async_remote_copy(
            src_ref=src,
            dst_ref=dst,
            send_sem=send_sem,
            recv_sem=recv_sem,
            device_id=(los_to, sky_to),
            device_id_type=MESH,
        )

    def wait_for(ref, sem):
        pltpu.make_async_copy(ref, ref, sem).wait()

    def paint_step(step, previous):
        for i in range(2):
            j = step * 2 + i
            z = lax.rem(z_here + order[0] + j, z_size)
            for x in range(X):
                planes = paint(z * X + x)
                for s in range(5):
                    carried = jnp.where(row == 0, pltpu.roll(previous[s], 4, 0), 0.0)
                    whole = (planes[s] + carried)[:4]
                    if s < 4:
                        grid[x, j, s] = whole
                    else:
                        grid_side[x, j] = whole
                previous = planes

        @pl.when(step == 0)
        def _():
            pl.semaphore_wait(barrier, 3 + 2 * X + z_size - 1)

        part = pl.ds(step * 2, 2)
        for k in (2, 1, 3, 0):
            x_to = (x_here + k) % X
            if k:
                remote(
                    grid.at[x_to, part],
                    rx.at[k - 1, part],
                    send_sems.at[0],
                    recv_x.at[step],
                    x_peer(k),
                    sky_here,
                ).start()
            remote(
                grid_side.at[x_to, part],
                rx_side.at[k, part],
                send_sems.at[0],
                recv_x.at[step],
                x_peer(k),
                sky_up,
            ).start()
        return tuple(previous)

    zero = jnp.zeros((8, LANES), F32)
    before = lax.rem(z_here + order[-1], z_size)
    lax.fori_loop(0, z_size // 2, paint_step, tuple(paint(before * X + X - 1)))

    for copy in fetched[5:]:
        copy.wait()
    rates[x_here, z_here] = by_row(rsd)
    for k in range(1, z_size):
        here = rates.at[x_here, z_here]
        remote(here, here, send_sems.at[1], recv_rates.at[0], z_peer(k), sky_here).start()

    for g in range(z_size // 2):
        wait_for(grid.at[:, pl.ds(2 * g, 2)], recv_x.at[g])
        for j in (2 * g, 2 * g + 1):
            for s in range(4):
                value = grid[x_here, j, s]
                for k in range(1, X):
                    value = value + rx[k - 1, j, s]
                if s == 0:
                    for k in range(X):
                        value = value + rx_side[k, j]
                total[j, s] = value
            k = order[j]
            if k:
                remote(
                    total.at[j], rz.at[k - 1], send_sems.at[2], recv_z, z_peer(k), sky_here
                ).start()

    wait_for(rates.at[0, pl.ds(0, z_size - 1)], recv_rates.at[0])
    for k in range(1, X):
        here = rates.at[x_here]
        remote(here, here, send_sems.at[3], recv_rates.at[1], x_peer(k), sky_here).start()

    exponent = by_row(bias)
    wait_for(rz, recv_z)
    for s in range(4):
        density = total[order.index(0), s]
        for k in range(1, z_size):
            density = density + rz[k - 1, s]
        mean = jnp.concatenate([selection[l, s : s + 1] for l in range(4)], axis=0)
        seen = jnp.concatenate([galaxies[l, s : s + 1] for l in range(4)], axis=0).astype(F32)
        shifted = density + 0.5
        intensity = mean * jnp.exp(exponent * jnp.log(shifted))
        field[x_here, z_here, s] = (1.0 - seen / intensity) * exponent * intensity / shifted

    def ring_distance(j):
        return min(j, z_size - j)

    nearest = sorted(range(z_size), key=ring_distance)
    for k in nearest[1:]:
        here = field.at[x_here, z_here]
        remote(
            here, here, send_sems.at[4], recv_cz.at[ring_distance(k) - 1], z_peer(k), sky_here
        ).start()
    arrived = {0}
    for j in nearest:
        if ring_distance(j) not in arrived:
            arrived.add(ring_distance(j))
            pieces = 1 if 2 * j == z_size else 2
            wait_for(rz.at[pl.ds(0, pieces)], recv_cz.at[ring_distance(j) - 1])
        z_from = (z_here + z_size - j) % z_size
        for k in (2, 1, 3, 0):
            if k:
                here = field.at[x_here, z_from]
                remote(
                    here, here, send_sems.at[5], recv_f.at[ring_distance(j)], x_peer(k), sky_here
                ).start()
            remote(
                field.at[x_here, z_from, 0],
                field_side.at[x_here, z_from],
                send_sems.at[5],
                recv_f.at[ring_distance(j)],
                x_peer(k),
                sky_down,
            ).start()
    wait_for(rates.at[pl.ds(0, X - 1)], recv_rates.at[1])

    def pull(z, x):
        t = z * X + x
        z_next, x_next = (z, x + 1) if x + 1 < X else ((z + 1) % z_size, 0)
        rows = []
        for s in range(5):
            if s < 4:
                value = jnp.concatenate([field[x, z, s], field[x_next, z_next, s]], axis=0)
            else:
                value = jnp.concatenate([field_side[x, z], field_side[x_next, z_next]], axis=0)
            rows += [value, pltpu.roll(value, LANES - 1, 1)]
        picked = jnp.dot(
            split(jnp.concatenate(rows, axis=0)), hot[t], preferred_element_type=F32
        )
        picked = picked[:80] + picked[80:]
        rate = jnp.concatenate([rates[x, z], jnp.zeros((4, LANES), F32)], axis=0)
        for slot in (0, 1):
            los, sky, deep, f_los, f_sky, f_deep = slot_rows(slots, slot, t)
            at, above = row == los, row == los + 1
            h_los = jnp.where(at, 1.0 - f_los, 0.0) + jnp.where(above, f_los, 0.0)
            d_los = jnp.where(above, 1.0, 0.0) - jnp.where(at, 1.0, 0.0)
            r_los = jnp.where(at, rate, 0.0)
            at, above = row == sky, row == sky + 1
            h_sky = jnp.where(at, 1.0 - f_sky, 0.0) + jnp.where(above, f_sky, 0.0)
            d_sky = jnp.where(above, 1.0, 0.0) - jnp.where(at, 1.0, 0.0)
            lanes = slice(slot * LANES, (slot + 1) * LANES)
            val, val_sky, val_deep = zero, zero, zero
            for s in range(5):
                here = picked[s * 16 : s * 16 + 8, lanes]
                step = picked[s * 16 + 8 : s * 16 + 16, lanes] - here
                mixed = here + f_deep * step
                val = val + h_sky[s : s + 1] * mixed
                val_sky = val_sky + d_sky[s : s + 1] * mixed
                val_deep = val_deep + h_sky[s : s + 1] * step
            g_los = jnp.sum(d_los * val, axis=0, keepdims=True)
            g_sky = jnp.sum(h_los * val_sky, axis=0, keepdims=True)
            g_deep = jnp.sum(h_los * val_deep, axis=0, keepdims=True)
            speed = jnp.sum(r_los, axis=0, keepdims=True) * g_los
            for r, value in enumerate((g_los, g_sky, g_deep, speed)):
                pulled[slot, r, pl.ds(t, 1), :] = value

    for g in range(z_size // 2):
        if g == 0:
            wait_for(grid.at[:, 0], recv_f.at[0])
        pieces = 1 if g + 1 == z_size // 2 else 2
        wait_for(grid.at[:, pl.ds(0, pieces)], recv_f.at[g + 1])
        for z in ((z_here + z_size - g - 1) % z_size, (z_here + g) % z_size):
            for x in range(X):
                pull(z, x)

    back = jnp.transpose(matrix).astype(BF16)
    parts = []
    for slot in (0, 1):
        parts.append(jnp.concatenate([pulled[slot, r] for r in range(4)], axis=1))
    result = jnp.dot(
        jnp.concatenate([back] * 3, axis=1),
        jnp.concatenate(thirds(jnp.concatenate(parts, axis=0)), axis=0),
        preferred_element_type=F32,
    )
    for b in range(blocks):
        for r in range(3):
            out_pos[r : r + 1, b * LANES : (b + 1) * LANES] = result[
                b : b + 1, r * LANES : (r + 1) * LANES
            ]
    out_vel[...] = result[:, 3 * LANES :]

    for sent, ref in enumerate(
        (grid, rates.at[0, pl.ds(0, z_size - 1)], rz, rates.at[pl.ds(0, X - 1)], rz, grid)
    ):
        wait_for(ref, send_sems.at[sent])


def on_device(
    part_cell,
    part_frac,
    los_offset,
    block_dest,
    block_count,
    selection,
    galaxy_counts,
    bias_exp,
    rsd_factor,
):
    los_size = lax.axis_size("los")
    z_size = los_size // X
    blocks = block_dest.shape[0]
    vmem = pl.BlockSpec(memory_space=pltpu.VMEM)
    hbm = pl.BlockSpec(memory_space=pltpu.HBM)
    dma = pltpu.SemaphoreType.DMA
    inputs = (
        block_dest.reshape(1, blocks),
        block_count.reshape(1, blocks),
        part_cell,
        part_frac,
        los_offset.reshape(blocks, LANES),
        bias_exp,
        rsd_factor,
        selection,
        galaxy_counts,
    )
    grad_pos, grad_vel = pl.pallas_call(
        kernel,
        out_shape=(
            pltpu.VMEM(part_frac.shape, F32),
            pltpu.VMEM((blocks, LANES), F32),
        ),
        in_specs=[hbm] * len(inputs),
        out_specs=(vmem, vmem),
        scratch_shapes=[
            *[
                (pltpu.SMEM if value.ndim == 1 else pltpu.VMEM)(value.shape, value.dtype)
                for value in inputs
            ],
            dma((len(inputs),)),
            pltpu.VMEM((6, blocks, LANES), F32),
            pltpu.VMEM((2, 6, los_size, LANES), F32),
            pltpu.VMEM((2, 4, los_size, LANES), F32),
            pltpu.VMEM((los_size, LANES, 2 * LANES), BF16),
            pltpu.VMEM((X, z_size, 4, 4, LANES), F32),
            pltpu.VMEM((X, z_size, 4, LANES), F32),
            pltpu.VMEM((X - 1, z_size, 4, 4, LANES), F32),
            pltpu.VMEM((X, z_size, 4, LANES), F32),
            pltpu.VMEM((z_size, 4, 4, LANES), F32),
            pltpu.VMEM((z_size - 1, 4, 4, LANES), F32),
            pltpu.VMEM((X, z_size, 4, 4, LANES), F32),
            pltpu.VMEM((X, z_size, 4, LANES), F32),
            pltpu.VMEM((X, z_size, 4, LANES), F32),
            dma((6,)),
            dma((z_size // 2,)),
            dma,
            dma((z_size // 2,)),
            dma((z_size // 2 + 1,)),
            dma((2,)),
        ],
        compiler_params=pltpu.CompilerParams(
            collective_id=0, has_side_effects=True
        ),
        name="adjoint",
    )(*inputs)
    return grad_pos, grad_vel.reshape(-1)


def solution(mesh):
    return jax.shard_map(
        on_device,
        mesh=mesh,
        in_specs=(
            P(None, ("los", "sky")),
            P(None, ("los", "sky")),
            P(("los", "sky")),
            P(("los", "sky")),
            P(("los", "sky")),
            P("los", "sky", None),
            P("los", "sky", None),
            P("los"),
            P("los"),
        ),
        out_specs=(P(None, ("los", "sky")), P(("los", "sky"))),
        check_vma=False,
    )
```

```python
import jax
import jax.numpy as jnp
from jax import lax
from jax.experimental import pallas as pl
from jax.experimental.pallas import tpu as pltpu
from jax.sharding import PartitionSpec as P

MESH = pl.DeviceIdType.MESH
F32 = jnp.float32
BF16 = jnp.bfloat16
LANES = 128
X = 4


def row_iota():
    return lax.broadcasted_iota(jnp.int32, (8, LANES), 0)


def split(values):
    high = values.astype(BF16)
    low = (values - high.astype(F32)).astype(BF16)
    return jnp.concatenate([high, low], axis=0)


def fetch(sources, targets, sems):
    copies = [
        pltpu.make_async_copy(source, target, sems.at[i])
        for i, (source, target) in enumerate(zip(sources, targets, strict=True))
    ]
    for copy in copies:
        copy.start()
    return copies


def thirds(values):
    high = values.astype(BF16)
    rest = values - high.astype(F32)
    middle = rest.astype(BF16)
    return [high, middle, (rest - middle.astype(F32)).astype(BF16)]


def slot_matrix(dest, counts, los_size):
    shape = (los_size, dest.shape[1])
    slab = lax.broadcasted_iota(jnp.int32, shape, 0)
    code = lax.broadcasted_iota(jnp.int32, shape, 1) * 256 + counts[...]
    code = jnp.where(slab == dest[...], code, -1).astype(F32)
    most = jnp.max(code, axis=1, keepdims=True)
    least = jnp.min(jnp.where(code < 0.0, 65536.0, code), axis=1, keepdims=True)
    single = least >= most
    first = jnp.where(code == least, 1.0, 0.0)
    second = jnp.where(single, 0.0, jnp.where(code == most, 1.0, 0.0))
    matrix = jnp.concatenate([first, second], axis=0)
    live = jnp.concatenate([jnp.maximum(least, 0.0), most], axis=0).astype(jnp.int32) & 255
    some = jnp.concatenate([most >= 0.0, jnp.logical_not(single)], axis=0)
    return matrix, jnp.where(some, live, 0)


def slot_rows(slots, slot, t):
    return [slots[slot, r, pl.ds(t, 1), :] for r in range(6)]


def one_hot_deep(deep):
    iota = lax.broadcasted_iota(jnp.int32, (LANES, LANES), 0).astype(F32).astype(BF16)
    one, none = jnp.ones((), BF16), jnp.zeros((), BF16)
    return jnp.where(iota == deep.astype(BF16), one, none)


def kernel(
    dest_in,
    counts_in,
    cell_in,
    frac_in,
    off_in,
    bias_in,
    rsd_in,
    selection_in,
    galaxies_in,
    out_pos,
    out_vel,
    dest,
    counts,
    cell,
    frac,
    off,
    bias,
    rsd,
    selection,
    galaxies,
    fetch_sems,
    rows_in,
    slots,
    pulled,
    grid,
    grid_side,
    rx,
    rx_side,
    total,
    rz,
    field,
    field_side,
    rates,
    send_sems,
    recv_x,
    recv_z,
    recv_cz,
    recv_f,
    recv_rates,
):
    z_size = grid.shape[1]
    sky_size = lax.axis_size("sky")
    los_size = X * z_size
    los_here = lax.axis_index("los")
    sky_here = lax.axis_index("sky")
    z_here = los_here // X
    x_here = los_here % X
    sky_up = (sky_here + 1) % sky_size
    sky_down = (sky_here + sky_size - 1) % sky_size

    def x_peer(k):
        return z_here * X + (x_here + k) % X

    def z_peer(k):
        return ((z_here + k) % z_size) * X + x_here

    fetched = fetch(
        (
            dest_in,
            counts_in,
            cell_in,
            frac_in,
            off_in,
            bias_in,
            rsd_in,
            selection_in,
            galaxies_in,
        ),
        (dest, counts, cell, frac, off, bias, rsd, selection, galaxies),
        fetch_sems,
    )
    barrier = pltpu.get_barrier_semaphore()
    for k in range(X):
        if k:
            pl.semaphore_signal(
                barrier, inc=1, device_id=(x_peer(k), sky_here), device_id_type=MESH
            )
        for sky_to in (sky_up, sky_down):
            pl.semaphore_signal(barrier, inc=1, device_id=(x_peer(k), sky_to), device_id_type=MESH)
    for k in range(1, z_size):
        pl.semaphore_signal(barrier, inc=1, device_id=(z_peer(k), sky_here), device_id_type=MESH)

    row4 = lax.broadcasted_iota(jnp.int32, (4, LANES), 0)

    def by_row(scalars):
        value = jnp.full((4, LANES), scalars[3], F32)
        for i in (0, 1, 2):
            value = jnp.where(row4 == i, scalars[i], value)
        return value

    row = row_iota().astype(F32)

    for copy in fetched[:5]:
        copy.wait()
    blocks = dest.shape[1]
    matrix, live = slot_matrix(dest, counts, los_size)
    for b in range(blocks):
        lanes = slice(b * LANES, (b + 1) * LANES)
        cells = cell[:, lanes].astype(F32)
        fracs = frac[:, lanes]
        for r in range(3):
            rows_in[r, b : b + 1, :] = cells[r : r + 1]
            rows_in[3 + r, b : b + 1, :] = fracs[r : r + 1]
    los_row = ((rows_in[0].astype(jnp.int32) + off[...]) & 3).astype(F32)
    sky_row = rows_in[1] - (sky_here * 4).astype(F32)
    parts = [los_row.astype(BF16), sky_row.astype(BF16), rows_in[2].astype(BF16)]
    for r in range(3):
        parts += thirds(rows_in[3 + r])
    placed = jnp.dot(
        matrix.astype(BF16), jnp.concatenate(parts, axis=1), preferred_element_type=F32
    )
    lane = lax.broadcasted_iota(jnp.int32, (2 * los_size, LANES), 1)
    for r in range(6):
        part = [placed[:, i * LANES : (i + 1) * LANES] for i in range(12)]
        if r < 3:
            value = jnp.where(lane < live, part[0], -8.0) if r == 0 else part[r]
        else:
            value = (part[3 * r - 6] + part[3 * r - 5]) + part[3 * r - 4]
        for slot in (0, 1):
            slots[slot, r] = value[slot * los_size : (slot + 1) * los_size]

    def paint(t):
        tables, hots = [], []
        for slot in (0, 1):
            los, sky, deep, f_los, f_sky, f_deep = slot_rows(slots, slot, t)
            h_los = jnp.where(row == los, 1.0 - f_los, 0.0) + jnp.where(row == los + 1, f_los, 0.0)
            h_sky = jnp.where(row == sky, 1.0 - f_sky, 0.0) + jnp.where(row == sky + 1, f_sky, 0.0)
            lower, upper = h_los * (1.0 - f_deep), h_los * f_deep
            parts = []
            for s in range(5):
                parts += [h_sky[s : s + 1] * lower, h_sky[s : s + 1] * upper]
            tables.append(split(jnp.concatenate(parts, axis=0)))
            hots.append(one_hot_deep(deep))
        result = lax.dot_general(
            jnp.concatenate(tables, axis=1),
            jnp.concatenate(hots, axis=1),
            (((1,), (1,)), ((), ())),
            preferred_element_type=F32,
        )
        result = result[:80] + result[80:]
        planes = []
        for s in range(5):
            lower, upper = result[s * 16 : s * 16 + 8], result[s * 16 + 8 : s * 16 + 16]
            planes.append(lower + pltpu.roll(upper, 1, 1))
        return planes

    order = [(z_size // 2 - 1 + j) % z_size for j in range(z_size)]

    def remote(src, dst, send_sem, recv_sem, los_to, sky_to):
        return pltpu.make_async_remote_copy(
            src_ref=src,
            dst_ref=dst,
            send_sem=send_sem,
            recv_sem=recv_sem,
            device_id=(los_to, sky_to),
            device_id_type=MESH,
        )

    def wait_for(ref, sem):
        pltpu.make_async_copy(ref, ref, sem).wait()

    def send_group(step):
        part = pl.ds(step * 2, 2)
        for k in (2, 1, 3, 0):
            x_to = (x_here + k) % X
            if k:
                remote(
                    grid.at[x_to, part],
                    rx.at[k - 1, part],
                    send_sems.at[0],
                    recv_x.at[step],
                    x_peer(k),
                    sky_here,
                ).start()
            remote(
                grid_side.at[x_to, part],
                rx_side.at[k, part],
                send_sems.at[0],
                recv_x.at[step],
                x_peer(k),
                sky_up,
            ).start()

    def paint_step(step, previous):
        for i in range(2):
            j = step * 2 + i
            z = lax.rem(z_here + order[0] + j, z_size)
            for x in range(X):
                planes = paint(z * X + x)
                for s in range(5):
                    carried = jnp.where(row == 0, pltpu.roll(previous[s], 4, 0), 0.0)
                    whole = (planes[s] + carried)[:4]
                    if s < 4:
                        grid[x, j, s] = whole
                    else:
                        grid_side[x, j] = whole
                previous = planes

        @pl.when(step == 1)
        def _():
            pl.semaphore_wait(barrier, 3 + 2 * X + z_size - 1)
            send_group(0)

        @pl.when(step >= 1)
        def _():
            send_group(step)

        return tuple(previous)

    zero = jnp.zeros((8, LANES), F32)
    before = lax.rem(z_here + order[-1], z_size)
    lax.fori_loop(0, z_size // 2, paint_step, tuple(paint(before * X + X - 1)))

    for copy in fetched[5:]:
        copy.wait()
    rates[x_here, z_here] = by_row(rsd)
    for k in range(1, z_size):
        here = rates.at[x_here, z_here]
        remote(here, here, send_sems.at[1], recv_rates.at[0], z_peer(k), sky_here).start()

    for g in range(z_size // 2):
        wait_for(grid.at[:, pl.ds(2 * g, 2)], recv_x.at[g])
        for j in (2 * g, 2 * g + 1):
            for s in range(4):
                value = grid[x_here, j, s]
                for k in range(1, X):
                    value = value + rx[k - 1, j, s]
                if s == 0:
                    for k in range(X):
                        value = value + rx_side[k, j]
                total[j, s] = value
            k = order[j]
            if k:
                remote(
                    total.at[j], rz.at[k - 1], send_sems.at[2], recv_z, z_peer(k), sky_here
                ).start()

    wait_for(rates.at[0, pl.ds(0, z_size - 1)], recv_rates.at[0])
    for k in range(1, X):
        here = rates.at[x_here]
        remote(here, here, send_sems.at[3], recv_rates.at[1], x_peer(k), sky_here).start()

    exponent = by_row(bias)
    wait_for(rz, recv_z)
    for s in range(4):
        density = total[order.index(0), s]
        for k in range(1, z_size):
            density = density + rz[k - 1, s]
        mean = jnp.concatenate([selection[l, s : s + 1] for l in range(4)], axis=0)
        seen = jnp.concatenate([galaxies[l, s : s + 1] for l in range(4)], axis=0).astype(F32)
        shifted = density + 0.5
        intensity = mean * jnp.exp(exponent * jnp.log(shifted))
        field[x_here, z_here, s] = (1.0 - seen / intensity) * exponent * intensity / shifted

    def ring_distance(j):
        return min(j, z_size - j)

    nearest = sorted(range(z_size), key=ring_distance)
    for k in nearest[1:]:
        here = field.at[x_here, z_here]
        remote(
            here, here, send_sems.at[4], recv_cz.at[ring_distance(k) - 1], z_peer(k), sky_here
        ).start()
    arrived = {0}
    for j in nearest:
        if ring_distance(j) not in arrived:
            arrived.add(ring_distance(j))
            pieces = 1 if 2 * j == z_size else 2
            wait_for(rz.at[pl.ds(0, pieces)], recv_cz.at[ring_distance(j) - 1])
        z_from = (z_here + z_size - j) % z_size
        for k in (2, 1, 3, 0):
            if k:
                here = field.at[x_here, z_from]
                remote(
                    here, here, send_sems.at[5], recv_f.at[ring_distance(j)], x_peer(k), sky_here
                ).start()
            remote(
                field.at[x_here, z_from, 0],
                field_side.at[x_here, z_from],
                send_sems.at[5],
                recv_f.at[ring_distance(j)],
                x_peer(k),
                sky_down,
            ).start()
    wait_for(rates.at[pl.ds(0, X - 1)], recv_rates.at[1])

    def pull(z, x):
        t = z * X + x
        z_next, x_next = (z, x + 1) if x + 1 < X else ((z + 1) % z_size, 0)
        rows = []
        for s in range(5):
            if s < 4:
                value = jnp.concatenate([field[x, z, s], field[x_next, z_next, s]], axis=0)
            else:
                value = jnp.concatenate([field_side[x, z], field_side[x_next, z_next]], axis=0)
            rows += [value, pltpu.roll(value, LANES - 1, 1)]
        both = [slot_rows(slots, slot, t) for slot in (0, 1)]
        picked = jnp.dot(
            split(jnp.concatenate(rows, axis=0)),
            jnp.concatenate([one_hot_deep(values[2]) for values in both], axis=1),
            preferred_element_type=F32,
        )
        picked = picked[:80] + picked[80:]
        rate = jnp.concatenate([rates[x, z], jnp.zeros((4, LANES), F32)], axis=0)
        for slot in (0, 1):
            los, sky, deep, f_los, f_sky, f_deep = both[slot]
            at, above = row == los, row == los + 1
            h_los = jnp.where(at, 1.0 - f_los, 0.0) + jnp.where(above, f_los, 0.0)
            d_los = jnp.where(above, 1.0, 0.0) - jnp.where(at, 1.0, 0.0)
            r_los = jnp.where(at, rate, 0.0)
            at, above = row == sky, row == sky + 1
            h_sky = jnp.where(at, 1.0 - f_sky, 0.0) + jnp.where(above, f_sky, 0.0)
            d_sky = jnp.where(above, 1.0, 0.0) - jnp.where(at, 1.0, 0.0)
            lanes = slice(slot * LANES, (slot + 1) * LANES)
            val, val_sky, val_deep = zero, zero, zero
            for s in range(5):
                here = picked[s * 16 : s * 16 + 8, lanes]
                step = picked[s * 16 + 8 : s * 16 + 16, lanes] - here
                mixed = here + f_deep * step
                val = val + h_sky[s : s + 1] * mixed
                val_sky = val_sky + d_sky[s : s + 1] * mixed
                val_deep = val_deep + h_sky[s : s + 1] * step
            g_los = jnp.sum(d_los * val, axis=0, keepdims=True)
            g_sky = jnp.sum(h_los * val_sky, axis=0, keepdims=True)
            g_deep = jnp.sum(h_los * val_deep, axis=0, keepdims=True)
            speed = jnp.sum(r_los, axis=0, keepdims=True) * g_los
            for r, value in enumerate((g_los, g_sky, g_deep, speed)):
                pulled[slot, r, pl.ds(t, 1), :] = value

    for g in range(z_size // 2):
        if g == 0:
            wait_for(grid.at[:, 0], recv_f.at[0])
        pieces = 1 if g + 1 == z_size // 2 else 2
        wait_for(grid.at[:, pl.ds(0, pieces)], recv_f.at[g + 1])
        ready = [(z_size - g - 1, x) for x in range(X)] + [(g, X - 1)]
        for d in {0: (0, 1), z_size // 2 - 1: ()}.get(g, (g + 1,)):
            ready += [(d, x) for x in range(X - 1)]
        for d, x in ready:
            pull((z_here + d) % z_size, x)

    back = jnp.transpose(matrix).astype(BF16)
    parts = []
    for slot in (0, 1):
        parts.append(jnp.concatenate([pulled[slot, r] for r in range(4)], axis=1))
    result = jnp.dot(
        jnp.concatenate([back] * 3, axis=1),
        jnp.concatenate(thirds(jnp.concatenate(parts, axis=0)), axis=0),
        preferred_element_type=F32,
    )
    for b in range(blocks):
        for r in range(3):
            out_pos[r : r + 1, b * LANES : (b + 1) * LANES] = result[
                b : b + 1, r * LANES : (r + 1) * LANES
            ]
    out_vel[...] = result[:, 3 * LANES :]

    for sent, ref in enumerate(
        (grid, rates.at[0, pl.ds(0, z_size - 1)], rz, rates.at[pl.ds(0, X - 1)], rz, grid)
    ):
        wait_for(ref, send_sems.at[sent])


def write_out(pos, vel, out_pos, out_vel, sems):
    for copy in fetch((pos, vel), (out_pos, out_vel), sems):
        copy.wait()


def on_device(
    part_cell,
    part_frac,
    los_offset,
    block_dest,
    block_count,
    selection,
    galaxy_counts,
    bias_exp,
    rsd_factor,
):
    los_size = lax.axis_size("los")
    z_size = los_size // X
    blocks = block_dest.shape[0]
    vmem = pl.BlockSpec(memory_space=pltpu.VMEM)
    hbm = pl.BlockSpec(memory_space=pltpu.HBM)
    dma = pltpu.SemaphoreType.DMA
    inputs = (
        block_dest.reshape(1, blocks),
        block_count.reshape(1, blocks),
        part_cell,
        part_frac,
        los_offset.reshape(blocks, LANES),
        bias_exp,
        rsd_factor,
        selection,
        galaxy_counts,
    )
    grad_pos, grad_vel = pl.pallas_call(
        kernel,
        out_shape=(
            pltpu.VMEM(part_frac.shape, F32),
            pltpu.VMEM((blocks, LANES), F32),
        ),
        in_specs=[hbm] * len(inputs),
        out_specs=(vmem, vmem),
        scratch_shapes=[
            *[
                (pltpu.SMEM if value.ndim == 1 else pltpu.VMEM)(value.shape, value.dtype)
                for value in inputs
            ],
            dma((len(inputs),)),
            pltpu.VMEM((6, blocks, LANES), F32),
            pltpu.VMEM((2, 6, los_size, LANES), F32),
            pltpu.VMEM((2, 4, los_size, LANES), F32),
            pltpu.VMEM((X, z_size, 4, 4, LANES), F32),
            pltpu.VMEM((X, z_size, 4, LANES), F32),
            pltpu.VMEM((X - 1, z_size, 4, 4, LANES), F32),
            pltpu.VMEM((X, z_size, 4, LANES), F32),
            pltpu.VMEM((z_size, 4, 4, LANES), F32),
            pltpu.VMEM((z_size - 1, 4, 4, LANES), F32),
            pltpu.VMEM((X, z_size, 4, 4, LANES), F32),
            pltpu.VMEM((X, z_size, 4, LANES), F32),
            pltpu.VMEM((X, z_size, 4, LANES), F32),
            dma((6,)),
            dma((z_size // 2,)),
            dma,
            dma((z_size // 2,)),
            dma((z_size // 2 + 1,)),
            dma((2,)),
        ],
        compiler_params=pltpu.CompilerParams(
            collective_id=0, has_side_effects=True
        ),
        name="adjoint",
    )(*inputs)
    grad_pos, grad_vel = pl.pallas_call(
        write_out,
        out_shape=(
            jax.ShapeDtypeStruct(grad_pos.shape, F32),
            jax.ShapeDtypeStruct(grad_vel.shape, F32),
        ),
        in_specs=[vmem, vmem],
        out_specs=(hbm, hbm),
        scratch_shapes=[dma((2,))],
        compiler_params=pltpu.CompilerParams(vmem_limit_bytes=1 << 20),
        name="write_out",
    )(grad_pos, grad_vel)
    return grad_pos, grad_vel.reshape(-1)


def solution(mesh):
    return jax.shard_map(
        on_device,
        mesh=mesh,
        in_specs=(
            P(None, ("los", "sky")),
            P(None, ("los", "sky")),
            P(("los", "sky")),
            P(("los", "sky")),
            P(("los", "sky")),
            P("los", "sky", None),
            P("los", "sky", None),
            P("los"),
            P("los"),
        ),
        out_specs=(P(None, ("los", "sky")), P(("los", "sky"))),
        check_vma=False,
    )
```

```python
import jax
import jax.numpy as jnp
from jax import lax
from jax.experimental import pallas as pl
from jax.experimental.pallas import tpu as pltpu
from jax.sharding import PartitionSpec as P

MESH = pl.DeviceIdType.MESH
F32 = jnp.float32
BF16 = jnp.bfloat16
LANES = 128
X = 4


def row_iota():
    return lax.broadcasted_iota(jnp.int32, (8, LANES), 0)


def split(values):
    high = values.astype(BF16)
    low = (values - high.astype(F32)).astype(BF16)
    return jnp.concatenate([high, low], axis=0)


def fetch(sources, targets, sems):
    copies = [
        pltpu.make_async_copy(source, target, sems.at[i])
        for i, (source, target) in enumerate(zip(sources, targets, strict=True))
    ]
    for copy in copies:
        copy.start()
    return copies


def thirds(values):
    high = values.astype(BF16)
    rest = values - high.astype(F32)
    middle = rest.astype(BF16)
    return [high, middle, (rest - middle.astype(F32)).astype(BF16)]


def slot_matrix(dest, counts, los_size):
    shape = (los_size, dest.shape[1])
    slab = lax.broadcasted_iota(jnp.int32, shape, 0)
    code = lax.broadcasted_iota(jnp.int32, shape, 1) * 256 + counts[...]
    code = jnp.where(slab == dest[...], code, -1).astype(F32)
    most = jnp.max(code, axis=1, keepdims=True)
    least = jnp.min(jnp.where(code < 0.0, 65536.0, code), axis=1, keepdims=True)
    single = least >= most
    first = jnp.where(code == least, 1.0, 0.0)
    second = jnp.where(single, 0.0, jnp.where(code == most, 1.0, 0.0))
    matrix = jnp.concatenate([first, second], axis=0)
    live = jnp.concatenate([jnp.maximum(least, 0.0), most], axis=0).astype(jnp.int32) & 255
    some = jnp.concatenate([most >= 0.0, jnp.logical_not(single)], axis=0)
    return matrix, jnp.where(some, live, 0)


def slot_rows(slots, slot, t):
    return [slots[slot, r, pl.ds(t, 1), :] for r in range(6)]


def one_hot_deep(deep):
    iota = lax.broadcasted_iota(jnp.int32, (LANES, LANES), 0).astype(F32).astype(BF16)
    one, none = jnp.ones((), BF16), jnp.zeros((), BF16)
    return jnp.where(iota == deep.astype(BF16), one, none)


def kernel(
    dest_in,
    counts_in,
    cell_in,
    frac_in,
    off_in,
    bias_in,
    rsd_in,
    selection_in,
    galaxies_in,
    out_pos,
    out_vel,
    dest,
    counts,
    cell,
    frac,
    off,
    bias,
    rsd,
    selection,
    galaxies,
    fetch_sems,
    rows_in,
    slots,
    pulled,
    grid,
    grid_side,
    rx,
    rx_side,
    total,
    rz,
    field,
    field_side,
    rates,
    send_sems,
    recv_x,
    recv_z,
    recv_cz,
    recv_f,
    recv_rates,
):
    z_size = grid.shape[1]
    sky_size = lax.axis_size("sky")
    los_size = X * z_size
    los_here = lax.axis_index("los")
    sky_here = lax.axis_index("sky")
    z_here = los_here // X
    x_here = los_here % X
    sky_up = (sky_here + 1) % sky_size
    sky_down = (sky_here + sky_size - 1) % sky_size

    def x_peer(k):
        return z_here * X + (x_here + k) % X

    def z_peer(k):
        return ((z_here + k) % z_size) * X + x_here

    fetched = fetch(
        (
            dest_in,
            counts_in,
            cell_in,
            frac_in,
            off_in,
            bias_in,
            rsd_in,
            selection_in,
            galaxies_in,
        ),
        (dest, counts, cell, frac, off, bias, rsd, selection, galaxies),
        fetch_sems,
    )
    barrier = pltpu.get_barrier_semaphore()
    for k in range(X):
        if k:
            pl.semaphore_signal(
                barrier, inc=1, device_id=(x_peer(k), sky_here), device_id_type=MESH
            )
        for sky_to in (sky_up, sky_down):
            pl.semaphore_signal(barrier, inc=1, device_id=(x_peer(k), sky_to), device_id_type=MESH)
    for k in range(1, z_size):
        pl.semaphore_signal(barrier, inc=1, device_id=(z_peer(k), sky_here), device_id_type=MESH)

    row4 = lax.broadcasted_iota(jnp.int32, (4, LANES), 0)

    def by_row(scalars):
        value = jnp.full((4, LANES), scalars[3], F32)
        for i in (0, 1, 2):
            value = jnp.where(row4 == i, scalars[i], value)
        return value

    row = row_iota().astype(F32)

    for copy in fetched[:5]:
        copy.wait()
    blocks = dest.shape[1]
    matrix, live = slot_matrix(dest, counts, los_size)
    for b in range(blocks):
        lanes = slice(b * LANES, (b + 1) * LANES)
        cells = cell[:, lanes].astype(F32)
        fracs = frac[:, lanes]
        for r in range(3):
            rows_in[r, b : b + 1, :] = cells[r : r + 1]
            rows_in[3 + r, b : b + 1, :] = fracs[r : r + 1]
    los_row = ((rows_in[0].astype(jnp.int32) + off[...]) & 3).astype(F32)
    sky_row = rows_in[1] - (sky_here * 4).astype(F32)
    parts = [los_row.astype(BF16), sky_row.astype(BF16), rows_in[2].astype(BF16)]
    for r in range(3):
        parts += thirds(rows_in[3 + r])
    placed = jnp.dot(
        matrix.astype(BF16), jnp.concatenate(parts, axis=1), preferred_element_type=F32
    )
    lane = lax.broadcasted_iota(jnp.int32, (2 * los_size, LANES), 1)
    for r in range(6):
        part = [placed[:, i * LANES : (i + 1) * LANES] for i in range(12)]
        if r < 3:
            value = jnp.where(lane < live, part[0], -8.0) if r == 0 else part[r]
        else:
            value = (part[3 * r - 6] + part[3 * r - 5]) + part[3 * r - 4]
        for slot in (0, 1):
            slots[slot, r] = value[slot * los_size : (slot + 1) * los_size]

    def paint(t):
        tables, hots = [], []
        for slot in (0, 1):
            los, sky, deep, f_los, f_sky, f_deep = slot_rows(slots, slot, t)
            h_los = jnp.where(row == los, 1.0 - f_los, 0.0) + jnp.where(row == los + 1, f_los, 0.0)
            h_sky = jnp.where(row == sky, 1.0 - f_sky, 0.0) + jnp.where(row == sky + 1, f_sky, 0.0)
            lower, upper = h_los * (1.0 - f_deep), h_los * f_deep
            parts = []
            for s in range(5):
                parts += [h_sky[s : s + 1] * lower, h_sky[s : s + 1] * upper]
            tables.append(split(jnp.concatenate(parts, axis=0)))
            hots.append(one_hot_deep(deep))
        result = lax.dot_general(
            jnp.concatenate(tables, axis=1),
            jnp.concatenate(hots, axis=1),
            (((1,), (1,)), ((), ())),
            preferred_element_type=F32,
        )
        result = result[:80] + result[80:]
        planes = []
        for s in range(5):
            lower, upper = result[s * 16 : s * 16 + 8], result[s * 16 + 8 : s * 16 + 16]
            planes.append(lower + pltpu.roll(upper, 1, 1))
        return planes

    order = [(z_size // 2 - 2 + j) % z_size for j in range(z_size)]

    def remote(src, dst, send_sem, recv_sem, los_to, sky_to):
        return pltpu.make_async_remote_copy(
            src_ref=src,
            dst_ref=dst,
            send_sem=send_sem,
            recv_sem=recv_sem,
            device_id=(los_to, sky_to),
            device_id_type=MESH,
        )

    def wait_for(ref, sem):
        pltpu.make_async_copy(ref, ref, sem).wait()

    def send_group(step):
        part = pl.ds(step * 2, 2)
        for k in (2, 1, 3, 0):
            x_to = (x_here + k) % X
            if k:
                remote(
                    grid.at[x_to, part],
                    rx.at[k - 1, part],
                    send_sems.at[0],
                    recv_x.at[step],
                    x_peer(k),
                    sky_here,
                ).start()
            remote(
                grid_side.at[x_to, part],
                rx_side.at[k, part],
                send_sems.at[0],
                recv_x.at[step],
                x_peer(k),
                sky_up,
            ).start()

    def paint_step(step, previous):
        for i in range(2):
            j = step * 2 + i
            z = lax.rem(z_here + order[0] + j, z_size)
            for x in range(X):
                planes = paint(z * X + x)
                for s in range(5):
                    carried = jnp.where(row == 0, pltpu.roll(previous[s], 4, 0), 0.0)
                    whole = (planes[s] + carried)[:4]
                    if s < 4:
                        grid[x, j, s] = whole
                    else:
                        grid_side[x, j] = whole
                previous = planes

        @pl.when(step == 0)
        def _():
            pl.semaphore_wait(barrier, 3 + 2 * X + z_size - 1)

        send_group(step)
        return tuple(previous)

    zero = jnp.zeros((8, LANES), F32)
    before = lax.rem(z_here + order[-1], z_size)
    lax.fori_loop(0, z_size // 2, paint_step, tuple(paint(before * X + X - 1)))

    for copy in fetched[5:]:
        copy.wait()
    rates[x_here, z_here] = by_row(rsd)
    for k in range(1, z_size):
        here = rates.at[x_here, z_here]
        remote(here, here, send_sems.at[1], recv_rates.at[0], z_peer(k), sky_here).start()

    for g in range(z_size // 2):
        wait_for(grid.at[:, pl.ds(2 * g, 2)], recv_x.at[g])
        for j in (2 * g, 2 * g + 1):
            for s in range(4):
                value = grid[x_here, j, s]
                for k in range(1, X):
                    value = value + rx[k - 1, j, s]
                if s == 0:
                    for k in range(X):
                        value = value + rx_side[k, j]
                total[j, s] = value
            k = order[j]
            if k:
                remote(
                    total.at[j], rz.at[k - 1], send_sems.at[2], recv_z, z_peer(k), sky_here
                ).start()

    wait_for(rates.at[0, pl.ds(0, z_size - 1)], recv_rates.at[0])
    for k in range(1, X):
        here = rates.at[x_here]
        remote(here, here, send_sems.at[3], recv_rates.at[1], x_peer(k), sky_here).start()

    exponent = by_row(bias)
    wait_for(rz, recv_z)
    for s in range(4):
        density = total[order.index(0), s]
        for k in range(1, z_size):
            density = density + rz[k - 1, s]
        mean = jnp.concatenate([selection[l, s : s + 1] for l in range(4)], axis=0)
        seen = jnp.concatenate([galaxies[l, s : s + 1] for l in range(4)], axis=0).astype(F32)
        shifted = density + 0.5
        intensity = mean * jnp.exp(exponent * jnp.log(shifted))
        field[x_here, z_here, s] = (1.0 - seen / intensity) * exponent * intensity / shifted

    def ring_distance(j):
        return min(j, z_size - j)

    def send_z(distance):
        for k in sorted({distance, z_size - distance}):
            here = field.at[x_here, z_here]
            remote(
                here, here, send_sems.at[4], recv_cz.at[distance - 1], z_peer(k), sky_here
            ).start()

    def send_x(distance, z_from, z_to):
        for k in (2, 1, 3, 0):
            los_to = z_to * X + (x_here + k) % X
            if k:
                here = field.at[x_here, z_from]
                remote(
                    here, here, send_sems.at[5], recv_f.at[distance], los_to, sky_here
                ).start()
            remote(
                field.at[x_here, z_from, 0],
                field_side.at[x_here, z_from],
                send_sems.at[5],
                recv_f.at[distance],
                los_to,
                sky_down,
            ).start()

    def wait_z(distance):
        pieces = 1 if 2 * distance == z_size else 2
        wait_for(rz.at[pl.ds(0, pieces)], recv_cz.at[distance - 1])

    straight = range(1, 2)
    passed_on = range(2, z_size // 2 + 1)
    for distance in passed_on:
        send_z(distance)
    send_x(0, z_here, z_here)
    for distance in straight:
        send_z(distance)
        for k in (distance, z_size - distance):
            send_x(distance, z_here, (z_here + k) % z_size)
    for distance in passed_on:
        wait_z(distance)
        for k in sorted({distance, z_size - distance}):
            send_x(distance, (z_here + k) % z_size, z_here)
    wait_for(rates.at[pl.ds(0, X - 1)], recv_rates.at[1])

    def pull(z, x):
        t = z * X + x
        z_next, x_next = (z, x + 1) if x + 1 < X else ((z + 1) % z_size, 0)
        rows = []
        for s in range(5):
            if s < 4:
                value = jnp.concatenate([field[x, z, s], field[x_next, z_next, s]], axis=0)
            else:
                value = jnp.concatenate([field_side[x, z], field_side[x_next, z_next]], axis=0)
            rows += [value, pltpu.roll(value, LANES - 1, 1)]
        both = [slot_rows(slots, slot, t) for slot in (0, 1)]
        picked = jnp.dot(
            split(jnp.concatenate(rows, axis=0)),
            jnp.concatenate([one_hot_deep(values[2]) for values in both], axis=1),
            preferred_element_type=F32,
        )
        picked = picked[:80] + picked[80:]
        rate = jnp.concatenate([rates[x, z], jnp.zeros((4, LANES), F32)], axis=0)
        for slot in (0, 1):
            los, sky, deep, f_los, f_sky, f_deep = both[slot]
            at, above = row == los, row == los + 1
            h_los = jnp.where(at, 1.0 - f_los, 0.0) + jnp.where(above, f_los, 0.0)
            d_los = jnp.where(above, 1.0, 0.0) - jnp.where(at, 1.0, 0.0)
            r_los = jnp.where(at, rate, 0.0)
            at, above = row == sky, row == sky + 1
            h_sky = jnp.where(at, 1.0 - f_sky, 0.0) + jnp.where(above, f_sky, 0.0)
            d_sky = jnp.where(above, 1.0, 0.0) - jnp.where(at, 1.0, 0.0)
            lanes = slice(slot * LANES, (slot + 1) * LANES)
            val, val_sky, val_deep = zero, zero, zero
            for s in range(5):
                here = picked[s * 16 : s * 16 + 8, lanes]
                step = picked[s * 16 + 8 : s * 16 + 16, lanes] - here
                mixed = here + f_deep * step
                val = val + h_sky[s : s + 1] * mixed
                val_sky = val_sky + d_sky[s : s + 1] * mixed
                val_deep = val_deep + h_sky[s : s + 1] * step
            g_los = jnp.sum(d_los * val, axis=0, keepdims=True)
            g_sky = jnp.sum(h_los * val_sky, axis=0, keepdims=True)
            g_deep = jnp.sum(h_los * val_deep, axis=0, keepdims=True)
            speed = jnp.sum(r_los, axis=0, keepdims=True) * g_los
            for r, value in enumerate((g_los, g_sky, g_deep, speed)):
                pulled[slot, r, pl.ds(t, 1), :] = value

    for g in range(z_size // 2):
        if g == 0:
            wait_for(grid.at[:, 0], recv_f.at[0])
        if g + 1 in straight:
            wait_z(g + 1)
        pieces = 1 if g + 1 == z_size // 2 else 2
        wait_for(grid.at[:, pl.ds(0, pieces)], recv_f.at[g + 1])
        ready = [(z_size - g - 1, x) for x in range(X)] + [(g, X - 1)]
        for d in {0: (0, 1), z_size // 2 - 1: ()}.get(g, (g + 1,)):
            ready += [(d, x) for x in range(X - 1)]
        for d, x in ready:
            pull((z_here + d) % z_size, x)

    back = jnp.transpose(matrix).astype(BF16)
    parts = []
    for slot in (0, 1):
        parts.append(jnp.concatenate([pulled[slot, r] for r in range(4)], axis=1))
    result = jnp.dot(
        jnp.concatenate([back] * 3, axis=1),
        jnp.concatenate(thirds(jnp.concatenate(parts, axis=0)), axis=0),
        preferred_element_type=F32,
    )
    for b in range(blocks):
        for r in range(3):
            out_pos[r : r + 1, b * LANES : (b + 1) * LANES] = result[
                b : b + 1, r * LANES : (r + 1) * LANES
            ]
    out_vel[...] = result[:, 3 * LANES :]

    for sent, ref in enumerate(
        (grid, rates.at[0, pl.ds(0, z_size - 1)], rz, rates.at[pl.ds(0, X - 1)], rz, grid)
    ):
        wait_for(ref, send_sems.at[sent])


def write_out(pos, vel, out_pos, out_vel, sems):
    for copy in fetch((pos, vel), (out_pos, out_vel), sems):
        copy.wait()


def on_device(
    part_cell,
    part_frac,
    los_offset,
    block_dest,
    block_count,
    selection,
    galaxy_counts,
    bias_exp,
    rsd_factor,
):
    los_size = lax.axis_size("los")
    z_size = los_size // X
    blocks = block_dest.shape[0]
    vmem = pl.BlockSpec(memory_space=pltpu.VMEM)
    hbm = pl.BlockSpec(memory_space=pltpu.HBM)
    dma = pltpu.SemaphoreType.DMA
    inputs = (
        block_dest.reshape(1, blocks),
        block_count.reshape(1, blocks),
        part_cell,
        part_frac,
        los_offset.reshape(blocks, LANES),
        bias_exp,
        rsd_factor,
        selection,
        galaxy_counts,
    )
    grad_pos, grad_vel = pl.pallas_call(
        kernel,
        out_shape=(
            pltpu.VMEM(part_frac.shape, F32),
            pltpu.VMEM((blocks, LANES), F32),
        ),
        in_specs=[hbm] * len(inputs),
        out_specs=(vmem, vmem),
        scratch_shapes=[
            *[
                (pltpu.SMEM if value.ndim == 1 else pltpu.VMEM)(value.shape, value.dtype)
                for value in inputs
            ],
            dma((len(inputs),)),
            pltpu.VMEM((6, blocks, LANES), F32),
            pltpu.VMEM((2, 6, los_size, LANES), F32),
            pltpu.VMEM((2, 4, los_size, LANES), F32),
            pltpu.VMEM((X, z_size, 4, 4, LANES), F32),
            pltpu.VMEM((X, z_size, 4, LANES), F32),
            pltpu.VMEM((X - 1, z_size, 4, 4, LANES), F32),
            pltpu.VMEM((X, z_size, 4, LANES), F32),
            pltpu.VMEM((z_size, 4, 4, LANES), F32),
            pltpu.VMEM((z_size - 1, 4, 4, LANES), F32),
            pltpu.VMEM((X, z_size, 4, 4, LANES), F32),
            pltpu.VMEM((X, z_size, 4, LANES), F32),
            pltpu.VMEM((X, z_size, 4, LANES), F32),
            dma((6,)),
            dma((z_size // 2,)),
            dma,
            dma((z_size // 2,)),
            dma((z_size // 2 + 1,)),
            dma((2,)),
        ],
        compiler_params=pltpu.CompilerParams(
            collective_id=0, has_side_effects=True
        ),
        name="adjoint",
    )(*inputs)
    grad_pos, grad_vel = pl.pallas_call(
        write_out,
        out_shape=(
            jax.ShapeDtypeStruct(grad_pos.shape, F32),
            jax.ShapeDtypeStruct(grad_vel.shape, F32),
        ),
        in_specs=[vmem, vmem],
        out_specs=(hbm, hbm),
        scratch_shapes=[dma((2,))],
        compiler_params=pltpu.CompilerParams(vmem_limit_bytes=1 << 20),
        name="write_out",
    )(grad_pos, grad_vel)
    return grad_pos, grad_vel.reshape(-1)


def solution(mesh):
    return jax.shard_map(
        on_device,
        mesh=mesh,
        in_specs=(
            P(None, ("los", "sky")),
            P(None, ("los", "sky")),
            P(("los", "sky")),
            P(("los", "sky")),
            P(("los", "sky")),
            P("los", "sky", None),
            P("los", "sky", None),
            P("los"),
            P("los"),
        ),
        out_specs=(P(None, ("los", "sky")), P(("los", "sky"))),
        check_vma=False,
    )
```

```python
import jax
import jax.numpy as jnp
from jax import lax
from jax.experimental import pallas as pl
from jax.experimental.pallas import tpu as pltpu
from jax.sharding import PartitionSpec as P

MESH = pl.DeviceIdType.MESH
F32 = jnp.float32
BF16 = jnp.bfloat16
LANES = 128
X = 4


def row_iota():
    return lax.broadcasted_iota(jnp.int32, (8, LANES), 0)


def split(values):
    high = values.astype(BF16)
    low = (values - high.astype(F32)).astype(BF16)
    return jnp.concatenate([high, low], axis=0)


def fetch(sources, targets, sems):
    copies = [
        pltpu.make_async_copy(source, target, sems.at[i])
        for i, (source, target) in enumerate(zip(sources, targets, strict=True))
    ]
    for copy in copies:
        copy.start()
    return copies


def thirds(values):
    high = values.astype(BF16)
    rest = values - high.astype(F32)
    middle = rest.astype(BF16)
    return [high, middle, (rest - middle.astype(F32)).astype(BF16)]


def slot_matrix(dest, counts, los_size):
    shape = (los_size, dest.shape[1])
    slab = lax.broadcasted_iota(jnp.int32, shape, 0)
    code = lax.broadcasted_iota(jnp.int32, shape, 1) * 256 + counts[...]
    code = jnp.where(slab == dest[...], code, -1).astype(F32)
    most = jnp.max(code, axis=1, keepdims=True)
    least = jnp.min(jnp.where(code < 0.0, 65536.0, code), axis=1, keepdims=True)
    single = least >= most
    first = jnp.where(code == least, 1.0, 0.0)
    second = jnp.where(single, 0.0, jnp.where(code == most, 1.0, 0.0))
    matrix = jnp.concatenate([first, second], axis=0)
    live = jnp.concatenate([jnp.maximum(least, 0.0), most], axis=0).astype(jnp.int32) & 255
    some = jnp.concatenate([most >= 0.0, jnp.logical_not(single)], axis=0)
    return matrix, jnp.where(some, live, 0)


def slot_rows(slots, slot, t):
    return [slots[slot, r, pl.ds(t, 1), :] for r in range(6)]


def one_hot_deep(deep):
    iota = lax.broadcasted_iota(jnp.int32, (LANES, LANES), 0).astype(F32).astype(BF16)
    one, none = jnp.ones((), BF16), jnp.zeros((), BF16)
    return jnp.where(iota == deep.astype(BF16), one, none)


def kernel(
    dest_in,
    counts_in,
    cell_in,
    frac_in,
    off_in,
    bias_in,
    rsd_in,
    selection_in,
    galaxies_in,
    out_pos,
    out_vel,
    dest,
    counts,
    cell,
    frac,
    off,
    bias,
    rsd,
    selection,
    galaxies,
    fetch_sems,
    rows_in,
    slots,
    pulled,
    grid,
    grid_side,
    rx,
    rx_side,
    total,
    rz,
    field,
    field_side,
    rates,
    send_sems,
    recv_x,
    recv_z,
    recv_cz,
    recv_f,
    recv_rates,
):
    z_size = grid.shape[1]
    sky_size = lax.axis_size("sky")
    los_size = X * z_size
    los_here = lax.axis_index("los")
    sky_here = lax.axis_index("sky")
    z_here = los_here // X
    x_here = los_here % X
    sky_up = (sky_here + 1) % sky_size
    sky_down = (sky_here + sky_size - 1) % sky_size

    def x_peer(k):
        return z_here * X + (x_here + k) % X

    def z_peer(k):
        return ((z_here + k) % z_size) * X + x_here

    fetched = fetch(
        (
            dest_in,
            counts_in,
            cell_in,
            frac_in,
            off_in,
            bias_in,
            rsd_in,
            selection_in,
            galaxies_in,
        ),
        (dest, counts, cell, frac, off, bias, rsd, selection, galaxies),
        fetch_sems,
    )
    barrier = pltpu.get_barrier_semaphore()
    for k in range(X):
        if k:
            pl.semaphore_signal(
                barrier, inc=1, device_id=(x_peer(k), sky_here), device_id_type=MESH
            )
        for sky_to in (sky_up, sky_down):
            pl.semaphore_signal(barrier, inc=1, device_id=(x_peer(k), sky_to), device_id_type=MESH)
    for k in range(1, z_size):
        pl.semaphore_signal(barrier, inc=1, device_id=(z_peer(k), sky_here), device_id_type=MESH)

    row4 = lax.broadcasted_iota(jnp.int32, (4, LANES), 0)

    def by_row(scalars):
        value = jnp.full((4, LANES), scalars[3], F32)
        for i in (0, 1, 2):
            value = jnp.where(row4 == i, scalars[i], value)
        return value

    row = row_iota().astype(F32)

    for copy in fetched[:5]:
        copy.wait()
    blocks = dest.shape[1]
    matrix, live = slot_matrix(dest, counts, los_size)
    for b in range(blocks):
        lanes = slice(b * LANES, (b + 1) * LANES)
        cells = cell[:, lanes].astype(F32)
        fracs = frac[:, lanes]
        for r in range(3):
            rows_in[r, b : b + 1, :] = cells[r : r + 1]
            rows_in[3 + r, b : b + 1, :] = fracs[r : r + 1]
    los_row = ((rows_in[0].astype(jnp.int32) + off[...]) & 3).astype(F32)
    sky_row = rows_in[1] - (sky_here * 4).astype(F32)
    parts = [los_row.astype(BF16), sky_row.astype(BF16), rows_in[2].astype(BF16)]
    for r in range(3):
        parts += thirds(rows_in[3 + r])
    placed = jnp.dot(
        matrix.astype(BF16), jnp.concatenate(parts, axis=1), preferred_element_type=F32
    )
    lane = lax.broadcasted_iota(jnp.int32, (2 * los_size, LANES), 1)
    for r in range(6):
        part = [placed[:, i * LANES : (i + 1) * LANES] for i in range(12)]
        if r < 3:
            value = jnp.where(lane < live, part[0], -8.0) if r == 0 else part[r]
        else:
            value = (part[3 * r - 6] + part[3 * r - 5]) + part[3 * r - 4]
        for slot in (0, 1):
            slots[slot, r] = value[slot * los_size : (slot + 1) * los_size]

    def paint(t):
        tables, hots = [], []
        for slot in (0, 1):
            los, sky, deep, f_los, f_sky, f_deep = slot_rows(slots, slot, t)
            h_los = jnp.where(row == los, 1.0 - f_los, jnp.where(row == los + 1, f_los, 0.0))
            h_sky = jnp.where(row == sky, 1.0 - f_sky, jnp.where(row == sky + 1, f_sky, 0.0))
            lower, upper = h_los * (1.0 - f_deep), h_los * f_deep
            parts = []
            for s in range(5):
                parts += [h_sky[s : s + 1] * lower, h_sky[s : s + 1] * upper]
            tables.append(split(jnp.concatenate(parts, axis=0)))
            hots.append(one_hot_deep(deep))
        result = lax.dot_general(
            jnp.concatenate(tables, axis=1),
            jnp.concatenate(hots, axis=1),
            (((1,), (1,)), ((), ())),
            preferred_element_type=F32,
        )
        result = result[:80] + result[80:]
        planes = []
        for s in range(5):
            lower, upper = result[s * 16 : s * 16 + 8], result[s * 16 + 8 : s * 16 + 16]
            planes.append(lower + pltpu.roll(upper, 1, 1))
        return planes

    order = [(z_size // 2 - 2 + j) % z_size for j in range(z_size)]

    def remote(src, dst, send_sem, recv_sem, los_to, sky_to):
        return pltpu.make_async_remote_copy(
            src_ref=src,
            dst_ref=dst,
            send_sem=send_sem,
            recv_sem=recv_sem,
            device_id=(los_to, sky_to),
            device_id_type=MESH,
        )

    def wait_for(ref, sem):
        pltpu.make_async_copy(ref, ref, sem).wait()

    def send_group(step):
        part = pl.ds(step * 2, 2)
        for k in (2, 1, 3, 0):
            x_to = (x_here + k) % X
            if k:
                remote(
                    grid.at[x_to, part],
                    rx.at[k - 1, part],
                    send_sems.at[0],
                    recv_x.at[step],
                    x_peer(k),
                    sky_here,
                ).start()
            remote(
                grid_side.at[x_to, part],
                rx_side.at[k, part],
                send_sems.at[0],
                recv_x.at[step],
                x_peer(k),
                sky_up,
            ).start()

    def paint_step(step, previous):
        for i in range(2):
            j = step * 2 + i
            z = lax.rem(z_here + order[0] + j, z_size)
            for x in range(X):
                planes = paint(z * X + x)
                for s in range(5):
                    carried = jnp.where(row == 0, pltpu.roll(previous[s], 4, 0), 0.0)
                    whole = (planes[s] + carried)[:4]
                    if s < 4:
                        grid[x, j, s] = whole
                    else:
                        grid_side[x, j] = whole
                previous = planes

        @pl.when(step == 0)
        def _():
            pl.semaphore_wait(barrier, 3 + 2 * X + z_size - 1)

        send_group(step)
        return tuple(previous)

    before = lax.rem(z_here + order[-1], z_size)
    lax.fori_loop(0, z_size // 2, paint_step, tuple(paint(before * X + X - 1)))

    for copy in fetched[5:]:
        copy.wait()
    rates[x_here, z_here] = by_row(rsd)
    for k in range(1, z_size):
        here = rates.at[x_here, z_here]
        remote(here, here, send_sems.at[1], recv_rates.at[0], z_peer(k), sky_here).start()

    for g in range(z_size // 2):
        wait_for(grid.at[:, pl.ds(2 * g, 2)], recv_x.at[g])
        for j in (2 * g, 2 * g + 1):
            for s in range(4):
                value = grid[x_here, j, s]
                for k in range(1, X):
                    value = value + rx[k - 1, j, s]
                if s == 0:
                    for k in range(X):
                        value = value + rx_side[k, j]
                total[j, s] = value
            k = order[j]
            if k:
                remote(
                    total.at[j], rz.at[k - 1], send_sems.at[2], recv_z, z_peer(k), sky_here
                ).start()

    wait_for(rates.at[0, pl.ds(0, z_size - 1)], recv_rates.at[0])
    for k in range(1, X):
        here = rates.at[x_here]
        remote(here, here, send_sems.at[3], recv_rates.at[1], x_peer(k), sky_here).start()

    exponent = by_row(bias)
    wait_for(rz, recv_z)
    for s in range(4):
        density = total[order.index(0), s]
        for k in range(1, z_size):
            density = density + rz[k - 1, s]
        mean = jnp.concatenate([selection[l, s : s + 1] for l in range(4)], axis=0)
        seen = jnp.concatenate([galaxies[l, s : s + 1] for l in range(4)], axis=0).astype(F32)
        shifted = density + 0.5
        intensity = mean * jnp.exp(exponent * jnp.log(shifted))
        field[x_here, z_here, s] = (1.0 - seen / intensity) * exponent * intensity / shifted

    def ring_distance(j):
        return min(j, z_size - j)

    def send_z(distance):
        for k in sorted({distance, z_size - distance}):
            here = field.at[x_here, z_here]
            remote(
                here, here, send_sems.at[4], recv_cz.at[distance - 1], z_peer(k), sky_here
            ).start()

    def send_x(distance, z_from, z_to):
        for k in (2, 1, 3):
            here = field.at[x_here, z_from]
            los_to = z_to * X + (x_here + k) % X
            remote(here, here, send_sems.at[5], recv_f.at[distance], los_to, sky_here).start()

    def send_side(distance, z_from, z_to):
        for k in (2, 1, 3, 0):
            remote(
                field.at[x_here, z_from, 0],
                field_side.at[x_here, z_from],
                send_sems.at[5],
                recv_f.at[distance],
                z_to * X + (x_here + k) % X,
                sky_down,
            ).start()

    def wait_z(distance):
        pieces = 1 if 2 * distance == z_size else 2
        wait_for(rz.at[pl.ds(0, pieces)], recv_cz.at[distance - 1])

    straight = range(1, 2)
    straight_sides = (4, 3, 2, 1)
    passed_on = range(2, z_size // 2 + 1)
    for distance in passed_on:
        send_z(distance)
    send_x(0, z_here, z_here)
    for distance in straight_sides:
        for k in sorted({distance, z_size - distance}):
            send_side(distance, z_here, (z_here + k) % z_size)
    send_side(0, z_here, z_here)
    for distance in straight:
        send_z(distance)
        for k in (distance, z_size - distance):
            send_x(distance, z_here, (z_here + k) % z_size)
    for distance in passed_on:
        wait_z(distance)
        for k in sorted({distance, z_size - distance}):
            z_from = (z_here + k) % z_size
            send_x(distance, z_from, z_here)
            if distance not in straight_sides:
                send_side(distance, z_from, z_here)
    wait_for(rates.at[pl.ds(0, X - 1)], recv_rates.at[1])

    def pull(z, x):
        t = z * X + x
        z_next, x_next = (z, x + 1) if x + 1 < X else ((z + 1) % z_size, 0)
        rows = []
        for s in range(5):
            if s < 4:
                value = jnp.concatenate([field[x, z, s], field[x_next, z_next, s]], axis=0)
            else:
                value = jnp.concatenate([field_side[x, z], field_side[x_next, z_next]], axis=0)
            rows += [value, pltpu.roll(value, LANES - 1, 1)]
        both = [slot_rows(slots, slot, t) for slot in (0, 1)]
        values = jnp.concatenate(rows, axis=0)
        high = values.astype(BF16)
        low = (values - high.astype(F32)).astype(BF16)
        one_hot = jnp.concatenate([one_hot_deep(slot[2]) for slot in both], axis=1)
        picked = jnp.dot(
            jnp.concatenate([high, low], axis=1),
            jnp.concatenate([one_hot, one_hot], axis=0),
            preferred_element_type=F32,
        )
        rate = jnp.concatenate([rates[x, z], jnp.zeros((4, LANES), F32)], axis=0)
        for slot in (0, 1):
            los, sky, deep, f_los, f_sky, f_deep = both[slot]
            at, above = row == los, row == los + 1
            h_los = jnp.where(at, 1.0 - f_los, jnp.where(above, f_los, 0.0))
            d_los = jnp.where(above, 1.0, jnp.where(at, -1.0, 0.0))
            r_los = jnp.where(at, rate, 0.0)
            at, above = row == sky, row == sky + 1
            h_sky = jnp.where(at, 1.0 - f_sky, jnp.where(above, f_sky, 0.0))
            d_sky = jnp.where(above, 1.0, jnp.where(at, -1.0, 0.0))
            lanes = slice(slot * LANES, (slot + 1) * LANES)
            sums = [None] * 3
            for s in range(5):
                here = picked[s * 16 : s * 16 + 8, lanes]
                step = picked[s * 16 + 8 : s * 16 + 16, lanes] - here
                mixed = here + f_deep * step
                terms = (
                    h_sky[s : s + 1] * mixed,
                    d_sky[s : s + 1] * mixed,
                    h_sky[s : s + 1] * step,
                )
                sums = [b if a is None else a + b for a, b in zip(sums, terms, strict=True)]
            parts = [d_los * sums[0], h_los * sums[1], h_los * sums[2], r_los]
            parts = [part + pltpu.roll(part, 4, 0) for part in parts]
            pairs = [jnp.where(row < 4.0, parts[i], parts[i + 1]) for i in (0, 2)]
            pairs = [pair + pltpu.roll(pair, 2, 0) for pair in pairs]
            pairs = [pair + pltpu.roll(pair, 1, 0) for pair in pairs]
            g_los, g_sky = pairs[0][3:4], pairs[0][7:8]
            g_deep, speed = pairs[1][3:4], pairs[1][7:8] * g_los
            for r, value in enumerate((g_los, g_sky, g_deep, speed)):
                pulled[slot, r, pl.ds(t, 1), :] = value

    for g in range(z_size // 2):
        if g == 0:
            wait_for(grid.at[:, 0], recv_f.at[0])
        if g + 1 in straight:
            wait_z(g + 1)
        pieces = 1 if g + 1 == z_size // 2 else 2
        wait_for(grid.at[:, pl.ds(0, pieces)], recv_f.at[g + 1])
        ready = [(z_size - g - 1, x) for x in range(X)] + [(g, X - 1)]
        for d in {0: (0, 1), z_size // 2 - 1: ()}.get(g, (g + 1,)):
            ready += [(d, x) for x in range(X - 1)]
        for d, x in ready:
            pull((z_here + d) % z_size, x)

    back = jnp.transpose(matrix).astype(BF16)
    parts = []
    for slot in (0, 1):
        parts.append(jnp.concatenate([pulled[slot, r] for r in range(4)], axis=1))
    result = jnp.dot(
        jnp.concatenate([back] * 3, axis=1),
        jnp.concatenate(thirds(jnp.concatenate(parts, axis=0)), axis=0),
        preferred_element_type=F32,
    )
    for b in range(blocks):
        for r in range(3):
            out_pos[r : r + 1, b * LANES : (b + 1) * LANES] = result[
                b : b + 1, r * LANES : (r + 1) * LANES
            ]
    out_vel[...] = result[:, 3 * LANES :]

    for sent, ref in enumerate(
        (grid, rates.at[0, pl.ds(0, z_size - 1)], rz, rates.at[pl.ds(0, X - 1)], rz, grid)
    ):
        wait_for(ref, send_sems.at[sent])


def write_out(pos, vel, out_pos, out_vel, sems):
    for copy in fetch((pos, vel), (out_pos, out_vel), sems):
        copy.wait()


def on_device(
    part_cell,
    part_frac,
    los_offset,
    block_dest,
    block_count,
    selection,
    galaxy_counts,
    bias_exp,
    rsd_factor,
):
    los_size = lax.axis_size("los")
    z_size = los_size // X
    blocks = block_dest.shape[0]
    vmem = pl.BlockSpec(memory_space=pltpu.VMEM)
    hbm = pl.BlockSpec(memory_space=pltpu.HBM)
    dma = pltpu.SemaphoreType.DMA
    inputs = (
        block_dest.reshape(1, blocks),
        block_count.reshape(1, blocks),
        part_cell,
        part_frac,
        los_offset.reshape(blocks, LANES),
        bias_exp,
        rsd_factor,
        selection,
        galaxy_counts,
    )
    grad_pos, grad_vel = pl.pallas_call(
        kernel,
        out_shape=(
            pltpu.VMEM(part_frac.shape, F32),
            pltpu.VMEM((blocks, LANES), F32),
        ),
        in_specs=[hbm] * len(inputs),
        out_specs=(vmem, vmem),
        scratch_shapes=[
            *[
                (pltpu.SMEM if value.ndim == 1 else pltpu.VMEM)(value.shape, value.dtype)
                for value in inputs
            ],
            dma((len(inputs),)),
            pltpu.VMEM((6, blocks, LANES), F32),
            pltpu.VMEM((2, 6, los_size, LANES), F32),
            pltpu.VMEM((2, 4, los_size, LANES), F32),
            pltpu.VMEM((X, z_size, 4, 4, LANES), F32),
            pltpu.VMEM((X, z_size, 4, LANES), F32),
            pltpu.VMEM((X - 1, z_size, 4, 4, LANES), F32),
            pltpu.VMEM((X, z_size, 4, LANES), F32),
            pltpu.VMEM((z_size, 4, 4, LANES), F32),
            pltpu.VMEM((z_size - 1, 4, 4, LANES), F32),
            pltpu.VMEM((X, z_size, 4, 4, LANES), F32),
            pltpu.VMEM((X, z_size, 4, LANES), F32),
            pltpu.VMEM((X, z_size, 4, LANES), F32),
            dma((6,)),
            dma((z_size // 2,)),
            dma,
            dma((z_size // 2,)),
            dma((z_size // 2 + 1,)),
            dma((2,)),
        ],
        compiler_params=pltpu.CompilerParams(
            collective_id=0, has_side_effects=True
        ),
        name="adjoint",
    )(*inputs)
    grad_pos, grad_vel = pl.pallas_call(
        write_out,
        out_shape=(
            jax.ShapeDtypeStruct(grad_pos.shape, F32),
            jax.ShapeDtypeStruct(grad_vel.shape, F32),
        ),
        in_specs=[vmem, vmem],
        out_specs=(hbm, hbm),
        scratch_shapes=[dma((2,))],
        compiler_params=pltpu.CompilerParams(vmem_limit_bytes=1 << 20),
        name="write_out",
    )(grad_pos, grad_vel)
    return grad_pos, grad_vel.reshape(-1)


def solution(mesh):
    return jax.shard_map(
        on_device,
        mesh=mesh,
        in_specs=(
            P(None, ("los", "sky")),
            P(None, ("los", "sky")),
            P(("los", "sky")),
            P(("los", "sky")),
            P(("los", "sky")),
            P("los", "sky", None),
            P("los", "sky", None),
            P("los"),
            P("los"),
        ),
        out_specs=(P(None, ("los", "sky")), P(("los", "sky"))),
        check_vma=False,
    )
```

```python
import jax
import jax.numpy as jnp
from jax import lax
from jax.experimental import pallas as pl
from jax.experimental.pallas import tpu as pltpu
from jax.sharding import PartitionSpec as P

MESH = pl.DeviceIdType.MESH
F32 = jnp.float32
BF16 = jnp.bfloat16
LANES = 128
X = 4


def row_iota():
    return lax.broadcasted_iota(jnp.int32, (8, LANES), 0)


def split(values):
    high = values.astype(BF16)
    low = (values - high.astype(F32)).astype(BF16)
    return jnp.concatenate([high, low], axis=0)


def fetch(sources, targets, sems):
    copies = [
        pltpu.make_async_copy(source, target, sems.at[i])
        for i, (source, target) in enumerate(zip(sources, targets, strict=True))
    ]
    for copy in copies:
        copy.start()
    return copies


def thirds(values):
    high = values.astype(BF16)
    rest = values - high.astype(F32)
    middle = rest.astype(BF16)
    return [high, middle, (rest - middle.astype(F32)).astype(BF16)]


def slot_matrix(dest, counts, los_size):
    shape = (los_size, dest.shape[1])
    slab = lax.broadcasted_iota(jnp.int32, shape, 0)
    code = lax.broadcasted_iota(jnp.int32, shape, 1) * 256 + counts[...]
    code = jnp.where(slab == dest[...], code, -1).astype(F32)
    most = jnp.max(code, axis=1, keepdims=True)
    least = jnp.min(jnp.where(code < 0.0, 65536.0, code), axis=1, keepdims=True)
    single = least >= most
    first = jnp.where(code == least, 1.0, 0.0)
    second = jnp.where(single, 0.0, jnp.where(code == most, 1.0, 0.0))
    matrix = jnp.concatenate([first, second], axis=0)
    live = jnp.concatenate([jnp.maximum(least, 0.0), most], axis=0).astype(jnp.int32) & 255
    some = jnp.concatenate([most >= 0.0, jnp.logical_not(single)], axis=0)
    return matrix, jnp.where(some, live, 0)


def slot_rows(slots, slot, t):
    return [slots[slot, r, pl.ds(t, 1), :] for r in range(6)]


def one_hot_deep(deep):
    iota = lax.broadcasted_iota(jnp.int32, (LANES, LANES), 0).astype(F32).astype(BF16)
    one, none = jnp.ones((), BF16), jnp.zeros((), BF16)
    return jnp.where(iota == deep.astype(BF16), one, none)


def kernel(
    dest_in,
    counts_in,
    cell_in,
    frac_in,
    off_in,
    bias_in,
    rsd_in,
    selection_in,
    galaxies_in,
    out_pos,
    out_vel,
    dest,
    counts,
    cell,
    frac,
    off,
    bias,
    rsd,
    selection,
    galaxies,
    fetch_sems,
    rows_in,
    slots,
    pulled,
    grid,
    grid_side,
    rx,
    rx_side,
    total,
    rz,
    field,
    field_side,
    rates,
    send_sems,
    recv_x,
    recv_z,
    recv_cz,
    recv_f,
    recv_rates,
):
    z_size = grid.shape[1]
    sky_size = lax.axis_size("sky")
    los_size = X * z_size
    los_here = lax.axis_index("los")
    sky_here = lax.axis_index("sky")
    z_here = los_here // X
    x_here = los_here % X
    sky_up = (sky_here + 1) % sky_size
    sky_down = (sky_here + sky_size - 1) % sky_size

    def x_peer(k):
        return z_here * X + (x_here + k) % X

    def z_peer(k):
        return ((z_here + k) % z_size) * X + x_here

    fetched = fetch(
        (
            dest_in,
            counts_in,
            cell_in,
            frac_in,
            off_in,
            bias_in,
            rsd_in,
            selection_in,
            galaxies_in,
        ),
        (dest, counts, cell, frac, off, bias, rsd, selection, galaxies),
        fetch_sems,
    )
    barrier = pltpu.get_barrier_semaphore()
    for k in range(X):
        if k:
            pl.semaphore_signal(
                barrier, inc=1, device_id=(x_peer(k), sky_here), device_id_type=MESH
            )
        for sky_to in (sky_up, sky_down):
            pl.semaphore_signal(barrier, inc=1, device_id=(x_peer(k), sky_to), device_id_type=MESH)
    for k in range(1, z_size):
        pl.semaphore_signal(barrier, inc=1, device_id=(z_peer(k), sky_here), device_id_type=MESH)

    row4 = lax.broadcasted_iota(jnp.int32, (4, LANES), 0)

    def by_row(scalars):
        value = jnp.full((4, LANES), scalars[3], F32)
        for i in (0, 1, 2):
            value = jnp.where(row4 == i, scalars[i], value)
        return value

    row = row_iota().astype(F32)

    for copy in fetched[:5]:
        copy.wait()
    blocks = dest.shape[1]
    matrix, live = slot_matrix(dest, counts, los_size)
    for b in range(blocks):
        lanes = slice(b * LANES, (b + 1) * LANES)
        cells = cell[:, lanes].astype(F32)
        fracs = frac[:, lanes]
        for r in range(3):
            rows_in[r, b : b + 1, :] = cells[r : r + 1]
            rows_in[3 + r, b : b + 1, :] = fracs[r : r + 1]
    los_row = ((rows_in[0].astype(jnp.int32) + off[...]) & 3).astype(F32)
    sky_row = rows_in[1] - (sky_here * 4).astype(F32)
    parts = [los_row.astype(BF16), sky_row.astype(BF16), rows_in[2].astype(BF16)]
    for r in range(3):
        parts += thirds(rows_in[3 + r])
    placed = jnp.dot(
        matrix.astype(BF16), jnp.concatenate(parts, axis=1), preferred_element_type=F32
    )
    lane = lax.broadcasted_iota(jnp.int32, (2 * los_size, LANES), 1)
    for r in range(6):
        part = [placed[:, i * LANES : (i + 1) * LANES] for i in range(12)]
        if r < 3:
            value = jnp.where(lane < live, part[0], -8.0) if r == 0 else part[r]
        else:
            value = (part[3 * r - 6] + part[3 * r - 5]) + part[3 * r - 4]
        for slot in (0, 1):
            slots[slot, r] = value[slot * los_size : (slot + 1) * los_size]

    def paint(t):
        tables, hots = [], []
        for slot in (0, 1):
            los, sky, deep, f_los, f_sky, f_deep = slot_rows(slots, slot, t)
            h_los = jnp.where(row == los, 1.0 - f_los, jnp.where(row == los + 1, f_los, 0.0))
            h_sky = jnp.where(row == sky, 1.0 - f_sky, jnp.where(row == sky + 1, f_sky, 0.0))
            lower, upper = h_los * (1.0 - f_deep), h_los * f_deep
            parts = []
            for s in range(5):
                parts += [h_sky[s : s + 1] * lower, h_sky[s : s + 1] * upper]
            tables.append(split(jnp.concatenate(parts, axis=0)))
            hots.append(one_hot_deep(deep))
        result = lax.dot_general(
            jnp.concatenate(tables, axis=1),
            jnp.concatenate(hots, axis=1),
            (((1,), (1,)), ((), ())),
            preferred_element_type=F32,
        )
        result = result[:80] + result[80:]
        planes = []
        for s in range(5):
            lower, upper = result[s * 16 : s * 16 + 8], result[s * 16 + 8 : s * 16 + 16]
            planes.append(lower + pltpu.roll(upper, 1, 1))
        return planes

    order = [(z_size // 2 - 2 + j) % z_size for j in range(z_size)]

    def remote(src, dst, send_sem, recv_sem, los_to, sky_to):
        return pltpu.make_async_remote_copy(
            src_ref=src,
            dst_ref=dst,
            send_sem=send_sem,
            recv_sem=recv_sem,
            device_id=(los_to, sky_to),
            device_id_type=MESH,
        )

    def wait_for(ref, sem):
        pltpu.make_async_copy(ref, ref, sem).wait()

    def send_group(step):
        part = pl.ds(step * 2, 2)
        for k in (2, 1, 3, 0):
            remote(
                grid_side.at[(x_here + k) % X, part],
                rx_side.at[k, part],
                send_sems.at[0],
                recv_x.at[step],
                x_peer(k),
                sky_up,
            ).start()
        for k in (2, 1, 3):
            remote(
                grid.at[(x_here + k) % X, part],
                rx.at[k - 1, part],
                send_sems.at[0],
                recv_x.at[step],
                x_peer(k),
                sky_here,
            ).start()

    def paint_step(step, previous):
        for i in range(2):
            j = step * 2 + i
            z = lax.rem(z_here + order[0] + j, z_size)
            for x in range(X):
                planes = paint(z * X + x)
                for s in range(5):
                    carried = jnp.where(row == 0, pltpu.roll(previous[s], 4, 0), 0.0)
                    whole = (planes[s] + carried)[:4]
                    if s < 4:
                        grid[x, j, s] = whole
                    else:
                        grid_side[x, j] = whole
                previous = planes

        @pl.when(step == 0)
        def _():
            pl.semaphore_wait(barrier, 3 + 2 * X + z_size - 1)

        send_group(step)
        return tuple(previous)

    before = lax.rem(z_here + order[-1], z_size)
    lax.fori_loop(0, z_size // 2, paint_step, tuple(paint(before * X + X - 1)))

    for copy in fetched[5:]:
        copy.wait()
    rates[x_here, z_here] = by_row(rsd)
    for k in range(1, z_size):
        here = rates.at[x_here, z_here]
        remote(here, here, send_sems.at[1], recv_rates.at[0], z_peer(k), sky_here).start()

    for g in range(z_size // 2):
        wait_for(grid.at[:, pl.ds(2 * g, 2)], recv_x.at[g])
        for j in (2 * g, 2 * g + 1):
            for s in range(4):
                value = grid[x_here, j, s]
                for k in range(1, X):
                    value = value + rx[k - 1, j, s]
                if s == 0:
                    for k in range(X):
                        value = value + rx_side[k, j]
                total[j, s] = value
            k = order[j]
            if k:
                remote(
                    total.at[j], rz.at[k - 1], send_sems.at[2], recv_z, z_peer(k), sky_here
                ).start()

    wait_for(rates.at[0, pl.ds(0, z_size - 1)], recv_rates.at[0])
    for k in range(1, X):
        here = rates.at[x_here]
        remote(here, here, send_sems.at[3], recv_rates.at[1], x_peer(k), sky_here).start()

    exponent = by_row(bias)
    wait_for(rz, recv_z)
    for s in range(4):
        density = total[order.index(0), s]
        for k in range(1, z_size):
            density = density + rz[k - 1, s]
        mean = jnp.concatenate([selection[l, s : s + 1] for l in range(4)], axis=0)
        seen = jnp.concatenate([galaxies[l, s : s + 1] for l in range(4)], axis=0).astype(F32)
        shifted = density + 0.5
        intensity = mean * jnp.exp(exponent * jnp.log(shifted))
        field[x_here, z_here, s] = (1.0 - seen / intensity) * exponent * intensity / shifted

    def ring_distance(j):
        return min(j, z_size - j)

    def send_z(distance):
        for k in sorted({distance, z_size - distance}):
            here = field.at[x_here, z_here]
            remote(
                here, here, send_sems.at[4], recv_cz.at[distance - 1], z_peer(k), sky_here
            ).start()

    def send_x(distance, z_from, z_to):
        for k in (2, 1, 3):
            here = field.at[x_here, z_from]
            los_to = z_to * X + (x_here + k) % X
            remote(here, here, send_sems.at[5], recv_f.at[distance], los_to, sky_here).start()

    def send_side(distance, z_from, z_to):
        for k in (2, 1, 3, 0):
            remote(
                field.at[x_here, z_from, 0],
                field_side.at[x_here, z_from],
                send_sems.at[5],
                recv_f.at[distance],
                z_to * X + (x_here + k) % X,
                sky_down,
            ).start()

    def wait_z(distance):
        pieces = 1 if 2 * distance == z_size else 2
        wait_for(rz.at[pl.ds(0, pieces)], recv_cz.at[distance - 1])

    straight = range(1, 2)
    straight_sides = (4, 3, 2, 1)
    passed_on = range(2, z_size // 2 + 1)
    for distance in passed_on:
        send_z(distance)
    send_x(0, z_here, z_here)
    for distance in straight_sides:
        for k in sorted({distance, z_size - distance}):
            send_side(distance, z_here, (z_here + k) % z_size)
    send_side(0, z_here, z_here)
    for distance in straight:
        send_z(distance)
        for k in (distance, z_size - distance):
            send_x(distance, z_here, (z_here + k) % z_size)
    for distance in passed_on:
        wait_z(distance)
        for k in sorted({distance, z_size - distance}):
            z_from = (z_here + k) % z_size
            send_x(distance, z_from, z_here)
            if distance not in straight_sides:
                send_side(distance, z_from, z_here)
    wait_for(rates.at[pl.ds(0, X - 1)], recv_rates.at[1])

    def pull(z, x):
        t = z * X + x
        z_next, x_next = (z, x + 1) if x + 1 < X else ((z + 1) % z_size, 0)
        rows = []
        for s in range(5):
            if s < 4:
                value = jnp.concatenate([field[x, z, s], field[x_next, z_next, s]], axis=0)
            else:
                value = jnp.concatenate([field_side[x, z], field_side[x_next, z_next]], axis=0)
            rows += [value, pltpu.roll(value, LANES - 1, 1)]
        both = [slot_rows(slots, slot, t) for slot in (0, 1)]
        values = jnp.concatenate(rows, axis=0)
        high = values.astype(BF16)
        low = (values - high.astype(F32)).astype(BF16)
        one_hot = jnp.concatenate([one_hot_deep(slot[2]) for slot in both], axis=1)
        picked = jnp.dot(
            jnp.concatenate([high, low], axis=1),
            jnp.concatenate([one_hot, one_hot], axis=0),
            preferred_element_type=F32,
        )
        rate = jnp.concatenate([rates[x, z], jnp.zeros((4, LANES), F32)], axis=0)
        for slot in (0, 1):
            los, sky, deep, f_los, f_sky, f_deep = both[slot]
            at, above = row == los, row == los + 1
            h_los = jnp.where(at, 1.0 - f_los, jnp.where(above, f_los, 0.0))
            d_los = jnp.where(above, 1.0, jnp.where(at, -1.0, 0.0))
            r_los = jnp.where(at, rate, 0.0)
            at, above = row == sky, row == sky + 1
            h_sky = jnp.where(at, 1.0 - f_sky, jnp.where(above, f_sky, 0.0))
            d_sky = jnp.where(above, 1.0, jnp.where(at, -1.0, 0.0))
            lanes = slice(slot * LANES, (slot + 1) * LANES)
            sums = [None] * 3
            for s in range(5):
                here = picked[s * 16 : s * 16 + 8, lanes]
                step = picked[s * 16 + 8 : s * 16 + 16, lanes] - here
                mixed = here + f_deep * step
                terms = (
                    h_sky[s : s + 1] * mixed,
                    d_sky[s : s + 1] * mixed,
                    h_sky[s : s + 1] * step,
                )
                sums = [b if a is None else a + b for a, b in zip(sums, terms, strict=True)]
            parts = [d_los * sums[0], h_los * sums[1], h_los * sums[2], r_los]
            parts = [part + pltpu.roll(part, 4, 0) for part in parts]
            pairs = [jnp.where(row < 4.0, parts[i], parts[i + 1]) for i in (0, 2)]
            pairs = [pair + pltpu.roll(pair, 2, 0) for pair in pairs]
            pairs = [pair + pltpu.roll(pair, 1, 0) for pair in pairs]
            g_los, g_sky = pairs[0][3:4], pairs[0][7:8]
            g_deep, speed = pairs[1][3:4], pairs[1][7:8] * g_los
            for r, value in enumerate((g_los, g_sky, g_deep, speed)):
                pulled[slot, r, pl.ds(t, 1), :] = value

    for g in range(z_size // 2):
        if g == 0:
            wait_for(grid.at[:, 0], recv_f.at[0])
        if g + 1 in straight:
            wait_z(g + 1)
        pieces = 1 if g + 1 == z_size // 2 else 2
        wait_for(grid.at[:, pl.ds(0, pieces)], recv_f.at[g + 1])
        ready = [(z_size - g - 1, x) for x in range(X)] + [(g, X - 1)]
        for d in {0: (0, 1), z_size // 2 - 1: ()}.get(g, (g + 1,)):
            ready += [(d, x) for x in range(X - 1)]
        for d, x in ready:
            pull((z_here + d) % z_size, x)

    back = jnp.transpose(matrix).astype(BF16)
    parts = []
    for slot in (0, 1):
        parts.append(jnp.concatenate([pulled[slot, r] for r in range(4)], axis=1))
    result = jnp.dot(
        jnp.concatenate([back] * 3, axis=1),
        jnp.concatenate(thirds(jnp.concatenate(parts, axis=0)), axis=0),
        preferred_element_type=F32,
    )
    for b in range(blocks):
        for r in range(3):
            out_pos[r : r + 1, b * LANES : (b + 1) * LANES] = result[
                b : b + 1, r * LANES : (r + 1) * LANES
            ]
    out_vel[...] = result[:, 3 * LANES :]

    for sent, ref in enumerate(
        (grid, rates.at[0, pl.ds(0, z_size - 1)], rz, rates.at[pl.ds(0, X - 1)], rz, grid)
    ):
        wait_for(ref, send_sems.at[sent])


def write_out(pos, vel, out_pos, out_vel, sems):
    for copy in fetch((pos, vel), (out_pos, out_vel), sems):
        copy.wait()


def on_device(
    part_cell,
    part_frac,
    los_offset,
    block_dest,
    block_count,
    selection,
    galaxy_counts,
    bias_exp,
    rsd_factor,
):
    los_size = lax.axis_size("los")
    z_size = los_size // X
    blocks = block_dest.shape[0]
    vmem = pl.BlockSpec(memory_space=pltpu.VMEM)
    hbm = pl.BlockSpec(memory_space=pltpu.HBM)
    dma = pltpu.SemaphoreType.DMA
    inputs = (
        block_dest.reshape(1, blocks),
        block_count.reshape(1, blocks),
        part_cell,
        part_frac,
        los_offset.reshape(blocks, LANES),
        bias_exp,
        rsd_factor,
        selection,
        galaxy_counts,
    )
    grad_pos, grad_vel = pl.pallas_call(
        kernel,
        out_shape=(
            pltpu.VMEM(part_frac.shape, F32),
            pltpu.VMEM((blocks, LANES), F32),
        ),
        in_specs=[hbm] * len(inputs),
        out_specs=(vmem, vmem),
        scratch_shapes=[
            *[
                (pltpu.SMEM if value.ndim == 1 else pltpu.VMEM)(value.shape, value.dtype)
                for value in inputs
            ],
            dma((len(inputs),)),
            pltpu.VMEM((6, blocks, LANES), F32),
            pltpu.VMEM((2, 6, los_size, LANES), F32),
            pltpu.VMEM((2, 4, los_size, LANES), F32),
            pltpu.VMEM((X, z_size, 4, 4, LANES), F32),
            pltpu.VMEM((X, z_size, 4, LANES), F32),
            pltpu.VMEM((X - 1, z_size, 4, 4, LANES), F32),
            pltpu.VMEM((X, z_size, 4, LANES), F32),
            pltpu.VMEM((z_size, 4, 4, LANES), F32),
            pltpu.VMEM((z_size - 1, 4, 4, LANES), F32),
            pltpu.VMEM((X, z_size, 4, 4, LANES), F32),
            pltpu.VMEM((X, z_size, 4, LANES), F32),
            pltpu.VMEM((X, z_size, 4, LANES), F32),
            dma((6,)),
            dma((z_size // 2,)),
            dma,
            dma((z_size // 2,)),
            dma((z_size // 2 + 1,)),
            dma((2,)),
        ],
        compiler_params=pltpu.CompilerParams(
            collective_id=0, has_side_effects=True
        ),
        name="adjoint",
    )(*inputs)
    grad_pos, grad_vel = pl.pallas_call(
        write_out,
        out_shape=(
            jax.ShapeDtypeStruct(grad_pos.shape, F32),
            jax.ShapeDtypeStruct(grad_vel.shape, F32),
        ),
        in_specs=[vmem, vmem],
        out_specs=(hbm, hbm),
        scratch_shapes=[dma((2,))],
        compiler_params=pltpu.CompilerParams(vmem_limit_bytes=1 << 20),
        name="write_out",
    )(grad_pos, grad_vel)
    return grad_pos, grad_vel.reshape(-1)


def solution(mesh):
    return jax.shard_map(
        on_device,
        mesh=mesh,
        in_specs=(
            P(None, ("los", "sky")),
            P(None, ("los", "sky")),
            P(("los", "sky")),
            P(("los", "sky")),
            P(("los", "sky")),
            P("los", "sky", None),
            P("los", "sky", None),
            P("los"),
            P("los"),
        ),
        out_specs=(P(None, ("los", "sky")), P(("los", "sky"))),
        check_vma=False,
    )
```
